512 devices in a mesh: grp: 2 (over y), tm: 32 (over z), chan: 4 (over x), sub: 2 (over core).
Axes of the slice: x: 4, y: 2, z: 32, core: 2. Of those that a mesh axis runs over, the one named last changes fastest.
The devices are a block of a 4x8x32 slice.
Arguments:
- signal: float32 [128, 1048576], P(('grp', 'chan', 'sub'), 'tm'), parts along dimension 0, may hold values from -24 to 24
- gap_mask: int32 [128, 64], P(('grp', 'chan', 'sub'), 'tm'), parts along dimension 0, may hold values from 0 to 1, as said below
- assignment: int32 [128], P(('grp', 'chan', 'sub')), parts along dimension 0, may hold values from 0 to 7, as said below
Outputs:
- peak_hold: float32 [128, 16384], P(('grp', 'chan', 'sub'), 'tm'), parts along dimension 0
- log_mean: float32 [128, 16384], P(('grp', 'chan', 'sub'), 'tm'), parts along dimension 0
- block_mean: float32 [16, 16384], P('grp', 'tm'), parts along dimension 0
The draws below stay inside these ranges and needn't reach their ends.
There are 2 independent parts, one for each index of `grp`. The reference program is written for one: setup_inputs(seed, part) draws one part's arguments, and reference() takes and returns one part's arrays. A program takes and returns all parts, laid end to end along the dimension named above; each array names one. Nothing has to cross between parts.
Inputs may be any that keep to these rules, and one draw needn't show every extreme that they name: `gap_mask`: every channel keeps at least one of its 64 segments. `assignment`: every block holds at least one channel.
All inputs are finite; a program needn't handle non-finite values.
Results may differ from the reference program's by a relative error of at most 0.000086.
Values sent between devices are 32-bit elements; how exact they have to be, the bound alone decides.
No kernel may reach another device: no remote copies, remote signals or barrier semaphores. Data moves between devices by JAX's collectives and lax.ppermute only.
A program may use at most 128 MiB of HBM per device.

```python
import math
import jax
import jax.numpy as jnp
from jax import lax

LA = 256
LB = 128
BLOCKS = 8
CHANNELS = 64
SEGS = 64
TOTAL = 1048576


def draw_signal(key, part):
    base_key = jax.random.fold_in(key, 11)
    noise_key, scale_key, level_key = jax.random.split(base_key, 3)
    noise = jnp.clip(jax.random.normal(noise_key, (CHANNELS, TOTAL), jnp.float32), -6.0, 6.0)
    scales = jnp.exp(jax.random.uniform(scale_key, (CHANNELS, 1), jnp.float32, jnp.log(0.5), jnp.log(2.0)))
    levels = jnp.exp(jax.random.uniform(level_key, (CHANNELS, SEGS), jnp.float32, jnp.log(0.5), jnp.log(2.0)))
    levels = jnp.repeat(levels, LA * LB // 2, axis=1)
    return (noise * scales * levels).astype(jnp.float32)


def draw_gap_mask(key, part):
    base_key = jax.random.fold_in(key, 23)
    rate_key, roll_key, forced_key = jax.random.split(base_key, 3)
    rates = jax.random.randint(rate_key, (CHANNELS, 1), 30, 96)
    rolls = jax.random.randint(roll_key, (CHANNELS, SEGS), 0, 100)
    forced = jax.random.randint(forced_key, (CHANNELS,), 0, SEGS)
    keep_flags = (rolls < rates) | (jnp.arange(SEGS)[None, :] == forced[:, None])
    return keep_flags.astype(jnp.int32)


def draw_assignment(key, part):
    base_key = jax.random.fold_in(key, 37)
    perm_key, pick_key = jax.random.split(base_key, 2)
    order = jax.random.permutation(perm_key, CHANNELS)
    picks = jax.random.randint(pick_key, (CHANNELS,), 0, BLOCKS)
    return picks.at[order[:BLOCKS]].set(jnp.arange(BLOCKS, dtype=jnp.int32)).astype(jnp.int32)


def setup_inputs(seed: int = 0, part: int = 0) -> dict:
    key_of = jax.random.split(jax.random.key(seed), 4)
    own_keys = jax.random.split(jax.random.fold_in(key_of[3], part), 4)
    signal = draw_signal(jax.random.fold_in(jax.random.fold_in(key_of[3], part), 71), part)
    gap_mask = draw_gap_mask(jax.random.fold_in(jax.random.fold_in(key_of[3], part), 71), part)
    assignment = draw_assignment(jax.random.fold_in(jax.random.fold_in(key_of[3], part), 71), part)
    return dict(signal=signal, gap_mask=gap_mask, assignment=assignment)


def reference(signal, gap_mask, assignment):
    seg_length = LA * LB
    half = seg_length // 2
    padded = jnp.concatenate([signal, jnp.zeros((CHANNELS, half), jnp.float32)], 1)
    hop_rows = padded.reshape(CHANNELS, SEGS + 1, half)
    samples = jnp.arange(seg_length)
    window = 0.5 - 0.5 * jnp.cos(2.0 * math.pi * samples / seg_length)
    norm_scale = 1.0 / (0.375 * seg_length)

    def one_channel(inputs):
        rows_here, keep_flags = inputs
        segments = jnp.concatenate([rows_here[:-1], rows_here[1:]], axis=-1) * window
        spectra = jnp.fft.fft(segments, axis=-1)[:, :half]
        powers = (jnp.real(spectra) ** 2 + jnp.imag(spectra) ** 2) * norm_scale
        weights = keep_flags.astype(jnp.float32)
        peak_one = jnp.max(powers * weights[:, None], axis=0)
        log_one = jnp.sum(weights[:, None] * jnp.log(0.25 + powers), axis=0) / jnp.sum(weights)
        return peak_one, log_one

    peak_hold, log_mean = lax.map(one_channel, (hop_rows, gap_mask))
    onehot = (assignment[None, :] == jnp.arange(BLOCKS)[:, None]).astype(jnp.float32)
    block_sum = jnp.dot(onehot, log_mean, precision=lax.Precision.HIGHEST)
    block_mean = block_sum / jnp.sum(onehot, axis=1)[:, None]
    return peak_hold, log_mean, block_mean
```

```python
import functools
import math

import jax
import jax.numpy as jnp
import numpy as np
from jax import lax
from jax.experimental import pallas as pl
from jax.experimental.pallas import tpu as pltpu
from jax.sharding import PartitionSpec as P

LA = 256
LB = 128
BLOCKS = 8
SEG = LA * LB
GROUP = 4
ROWS = 144
LANES = 128


def split(x):
    high = x.astype(jnp.bfloat16)
    return high, (x - high.astype(jnp.float32)).astype(jnp.bfloat16)


def split_np(x):
    high = x.astype(np.float32).astype(jnp.bfloat16)
    low = (x - high.astype(np.float64)).astype(np.float32).astype(jnp.bfloat16)
    return high, low


@functools.lru_cache
def tables(shards):
    k1 = np.arange(ROWS)[:, None]
    angle = 2 * math.pi * ((k1 * np.arange(LA)[None, :]) % LA) / LA
    live = k1 <= LA // 2
    first = np.concatenate([np.cos(angle) * live, -np.sin(angle) * live], axis=0)
    high, low = split_np(first)
    first = np.concatenate([high, high, low], axis=1)
    angle = 2 * math.pi * (k1 * np.arange(LB)[None, :]) / SEG
    scale = math.sqrt(1.0 / (0.375 * SEG)) * live
    twiddle = np.stack([np.cos(angle) * scale, -np.sin(angle) * scale]).astype(np.float32)
    own = LB // 2 // shards
    d = np.arange(shards)
    k2 = [own * d + e for e in range(own)] + [LB - 1 - own * d - e for e in range(own)]
    k2 = np.concatenate(k2)[None, :]
    angle = 2 * math.pi * ((np.arange(LB)[:, None] * k2) % LB) / LB
    c, s = np.cos(angle), -np.sin(angle)
    second = np.concatenate([np.concatenate([c, s], 1), np.concatenate([-s, c], 1)], 0)
    high, low = split_np(second)
    second = np.concatenate([high, high, low], axis=0)
    n = np.arange(SEG)
    window = (0.5 - 0.5 * np.cos(2 * math.pi * n / SEG)).reshape(LA, LB).astype(np.float32)
    return first, second, twiddle, window


def pack_kernel(per, mask_ref, x_ref, o_ref, a_ref, b_ref, c_ref, h_ref, cnt_ref):
    me = lax.axis_index("tm")
    channels = GROUP * per
    rows = x_ref.shape[0] // channels
    half = rows // 2
    even = lax.rem(me, 2) == 0

    def masks(ref, at, first):
        ref[at : at + 8, :] = jnp.zeros((8, LANES), jnp.float32)
        for c in range(per):
            for s in range(2):
                value = mask_ref[first + c, s].astype(jnp.float32)
                ref[at + 2 * c + s : at + 2 * c + s + 1, :] = jnp.full((1, LANES), value)

    for ref, shift in ((a_ref, 1), (b_ref, GROUP - 1), (c_ref, 2), (o_ref, 0)):
        first = per * lax.rem(me + shift, GROUP)
        for c in range(per):
            ref[c * rows : (c + 1) * rows, :] = x_ref[pl.ds(first + c, rows, stride=channels), :]
        masks(ref, per * rows, first)
    first = per * lax.rem(me + jnp.where(even, GROUP - 1, 1), GROUP)
    start = jnp.where(even, half * channels, 0)
    for c in range(per):
        h_ref[c * half : (c + 1) * half, :] = x_ref[
            pl.ds(start + first + c, half, stride=channels), :
        ]
    masks(h_ref, per * half, first)
    lane = lax.broadcasted_iota(jnp.int32, (1, LANES), 1)
    kept = jnp.zeros((1, LANES), jnp.float32)
    for c in range(channels):
        total = (mask_ref[c, 0] + mask_ref[c, 1]).astype(jnp.float32)
        kept = jnp.where(lane == c, total, kept)
    for d in range(cnt_ref.shape[0]):
        cnt_ref[d] = kept


def spectra_kernel(
    per, shards, o_ref, a_ref, b_ref, c_ref, h_ref, f_ref, w_ref, tw_ref, win_ref, out_ref
):
    me = lax.axis_index("tm")
    even = lax.rem(me, 2) == 0
    rows = (o_ref.shape[0] - 8) // per
    half = rows // 2
    parts = 2 * (LB // 2 // shards)
    lines = 2 * parts * per
    c_index = lax.rem(me + jnp.where(even, 2, shards - 2), shards)
    after_o = jnp.where(me == shards - 1, 0.0, 1.0)
    before_o = jnp.where(me == 0, 0.0, 1.0)
    before_c = jnp.where(c_index == 0, 0.0, 1.0)
    y_index = lax.rem(me + jnp.where(even, 3, shards - 1), shards)
    before_y = jnp.where(y_index == 0, 0.0, 1.0)
    swap = (lax.broadcasted_iota(jnp.int32, (8, LANES), 0) == 0) & (
        lax.broadcasted_iota(jnp.int32, (8, LANES), 1) >= LB // 2
    )

    def one_channel(c, carry):
        base = pl.multiple_of(c * rows, rows)
        h_base = pl.multiple_of(c * half, half)

        def halves(ref):
            return ref[pl.ds(base, half), :], ref[pl.ds(base + half, half), :]

        def weight(ref, s, at):
            return ref[pl.ds(at + 2 * c + s, 1), :]

        mask_at, h_mask_at = per * rows, per * half
        o0, o1 = halves(o_ref)
        a0, a1 = halves(a_ref)
        b0, b1 = halves(b_ref)
        c0, c1 = halves(c_ref)
        h = h_ref[pl.ds(h_base, half), :]
        x1 = jnp.where(even, b1, h)
        y = jnp.where(even, h, a0)
        x_weight = jnp.where(even, weight(b_ref, 1, mask_at), weight(h_ref, 1, h_mask_at))
        pairs = (
            ((a0, a1, None, weight(a_ref, 0, mask_at)), (a1, o0, before_o, weight(a_ref, 1, mask_at))),
            ((o0, o1, None, weight(o_ref, 0, mask_at)), (o1, b0, after_o, weight(o_ref, 1, mask_at))),
            ((b0, b1, None, weight(b_ref, 0, mask_at)), (x1, c0, before_c, x_weight)),
            ((c0, c1, None, weight(c_ref, 0, mask_at)), (c1, y, before_y, weight(c_ref, 1, mask_at))),
        )
        peak = log_sum = None
        for pair in pairs:
            framed = []
            for head, tail, live, _ in pair:
                tail = tail * win_ref[half:, :]
                if live is not None:
                    tail = tail * live
                framed.append(jnp.concatenate([head * win_ref[:half, :], tail], axis=0))
            high, low = split(jnp.concatenate(framed, axis=1))
            mid = jnp.dot(
                f_ref[...],
                jnp.concatenate([high, low, high], axis=0),
                preferred_element_type=jnp.float32,
            )
            turned = []
            for s in range(2):
                re = mid[:ROWS, s * LB : (s + 1) * LB]
                im = mid[ROWS:, s * LB : (s + 1) * LB]
                turned.append(
                    jnp.concatenate(
                        [re * tw_ref[0] - im * tw_ref[1], re * tw_ref[1] + im * tw_ref[0]], axis=1
                    )
                )
            high, low = split(jnp.concatenate(turned, axis=0))
            out = jnp.dot(
                jnp.concatenate([high, low, high], axis=1),
                w_ref[...],
                preferred_element_type=jnp.float32,
            )
            powers = out[:, :LB] * out[:, :LB] + out[:, LB:] * out[:, LB:]
            for s in range(2):
                mine = powers[s * ROWS : (s + 1) * ROWS]
                first = jnp.where(swap, mine[LA // 2 : LA // 2 + 8], mine[:8])
                mine = jnp.concatenate([first, mine[8 : LA // 2]], axis=0)
                keep = pair[s][3]
                kept_power = keep * mine
                kept_log = keep * jnp.log(0.25 + mine)
                peak = kept_power if peak is None else jnp.maximum(peak, kept_power)
                log_sum = kept_log if log_sum is None else log_sum + kept_log
        for kind, value in enumerate((peak, log_sum)):
            turned = jnp.transpose(value)
            for i in range(parts):
                out_ref[pl.ds(kind * parts * per + i * per + c, shards, stride=lines), :] = turned[
                    i * shards : (i + 1) * shards
                ]
        return carry

    lax.fori_loop(0, per, one_channel, 0)


def finish_kernel(per, own, assign_ref, z_ref, cnt_ref, peak_ref, log_ref, part_ref):
    channels = GROUP * per
    parts = 2 * own
    lines = 2 * parts * per
    shards = z_ref.shape[0] // lines
    lane = lax.broadcasted_iota(jnp.int32, (channels, LANES), 1)
    line = lax.broadcasted_iota(jnp.int32, (channels, LANES), 0)
    kept_row = jnp.sum(cnt_ref[...].reshape(shards, LANES), axis=0, keepdims=True)
    kept = jnp.sum(jnp.where(lane == line, kept_row, 0.0), axis=1, keepdims=True)
    back = jnp.where(lane == 0, 0, LANES - lane)

    def joined(kind, op):
        size = parts * per
        sets = []
        for r in range(GROUP):
            total = None
            for q in range(shards // GROUP):
                at = (GROUP * q + r) * lines + kind * size
                term = z_ref[at : at + size, :]
                total = term if total is None else op(total, term)
            sets.append(total)
        pieces = []
        for e in range(own):
            for i, mirrored in ((e, False), (own + e, True)):
                piece = jnp.concatenate([t[i * per : (i + 1) * per] for t in sets], axis=0)
                if mirrored:
                    piece = jnp.take_along_axis(piece, back, axis=1)
                pieces.append(piece)
        return jnp.concatenate(pieces, axis=1)

    peak_ref[...] = joined(0, jnp.maximum)
    log_mean = joined(1, jnp.add) / kept
    log_ref[...] = log_mean
    bins = log_mean.shape[1]
    block = lax.broadcasted_iota(jnp.int32, (BLOCKS, bins), 0)
    block_small = lax.broadcasted_iota(jnp.int32, (BLOCKS, LANES), 0)
    sums = jnp.zeros((BLOCKS, bins), jnp.float32)
    counts = jnp.zeros((BLOCKS, LANES), jnp.float32)
    for c in range(channels):
        sums = sums + jnp.where(block == assign_ref[c], log_mean[c : c + 1], 0.0)
        counts = counts + jnp.where(block_small == assign_ref[c], 1.0, 0.0)
    both = jnp.concatenate([sums, counts], axis=1)
    for p in range(part_ref.shape[0]):
        part_ref[p] = both


def blocks_kernel(parts_ref, out_ref):
    total = parts_ref[0]
    for p in range(1, parts_ref.shape[0]):
        total = total + parts_ref[p]
    bins = out_ref.shape[1]
    out_ref[...] = total[:, :bins] / total[:, bins : bins + 1]


VMEM = pl.BlockSpec(memory_space=pltpu.VMEM)
SMEM = pl.BlockSpec(memory_space=pltpu.SMEM)
PARAMS = pltpu.CompilerParams(vmem_limit_bytes=48 * 1024 * 1024)


def f32(*shape):
    return jax.ShapeDtypeStruct(shape, jnp.float32)


def on_device(signal, gap_mask, assignment):
    channels, local_time = signal.shape
    shards = lax.axis_size("tm")
    per = channels // GROUP
    rows = local_time // LANES
    half_bins = SEG // 2
    bins = half_bins // shards
    own = LB // 2 // shards
    lines = 2 * 2 * own * per
    first, second, twiddle, window = tables(shards)

    lined = signal.reshape(channels, rows, LANES).transpose(1, 0, 2).reshape(-1, LANES)
    size, small = per * rows + 8, per * rows // 2 + 8
    o, a, b, c, h, cnt = pl.pallas_call(
        functools.partial(pack_kernel, per),
        out_shape=[f32(size, LANES)] * 4 + [f32(small, LANES), f32(shards, 1, LANES)],
        in_specs=[SMEM, VMEM],
        out_specs=[VMEM] * 6,
        compiler_params=PARAMS,
        name="pack",
    )(gap_mask, lined)

    def moved(x, by):
        return lax.ppermute(x, "tm", [(i, (i + by(i)) % shards) for i in range(shards)])

    a = moved(a, lambda i: 1)
    b = moved(b, lambda i: -1)
    c = moved(c, lambda i: 2 if i % 2 else -2)
    h = moved(h, lambda i: -3 if i % 2 else 3)
    cnt = lax.all_to_all(cnt, "tm", 0, 0, tiled=True)

    sums = pl.pallas_call(
        functools.partial(spectra_kernel, per, shards),
        out_shape=f32(shards * lines, LANES),
        in_specs=[VMEM] * 9,
        out_specs=VMEM,
        compiler_params=PARAMS,
        cost_estimate=pl.CostEstimate(
            flops=4_000_000_000, bytes_accessed=4_000_000, transcendentals=300_000
        ),
        name="spectra",
    )(o, a, b, c, h, jnp.asarray(first), jnp.asarray(second), twiddle, window)
    sums = lax.all_to_all(sums.reshape(shards, lines, LANES), "tm", 0, 0, tiled=True)
    peers = lax.axis_size(("chan", "sub"))
    peak_hold, log_mean, part = pl.pallas_call(
        functools.partial(finish_kernel, per, own),
        out_shape=[f32(channels, bins), f32(channels, bins), f32(peers, BLOCKS, bins + LANES)],
        in_specs=[SMEM, VMEM, VMEM],
        out_specs=[VMEM] * 3,
        compiler_params=PARAMS,
        name="finish",
    )(assignment, sums.reshape(shards * lines, LANES), cnt)
    part = lax.all_to_all(part, ("chan", "sub"), 0, 0, tiled=True)
    block_mean = pl.pallas_call(
        blocks_kernel,
        out_shape=f32(BLOCKS, bins),
        in_specs=[VMEM],
        out_specs=VMEM,
        compiler_params=PARAMS,
        name="blocks",
    )(part)
    return peak_hold, log_mean, block_mean


def solution(mesh):
    in_specs = (
        P(("grp", "chan", "sub"), "tm"),
        P(("grp", "chan", "sub"), "tm"),
        P(("grp", "chan", "sub")),
    )
    out_specs = (P(("grp", "chan", "sub"), "tm"), P(("grp", "chan", "sub"), "tm"), P("grp", "tm"))
    return jax.shard_map(
        on_device, mesh=mesh, in_specs=in_specs, out_specs=out_specs, check_vma=False
    )
```

```python
import functools
import math

import jax
import jax.numpy as jnp
import numpy as np
from jax import lax
from jax.experimental import pallas as pl
from jax.experimental.pallas import tpu as pltpu
from jax.sharding import PartitionSpec as P

LA = 256
LB = 128
BLOCKS = 8
SEG = LA * LB
GROUP = 4
ROWS = 144
LANES = 128


def split(x):
    high = x.astype(jnp.bfloat16)
    return high, (x - high.astype(jnp.float32)).astype(jnp.bfloat16)


def split_np(x):
    high = x.astype(np.float32).astype(jnp.bfloat16)
    low = (x - high.astype(np.float64)).astype(np.float32).astype(jnp.bfloat16)
    return high, low


@functools.lru_cache
def tables(shards):
    k1 = np.arange(ROWS)[:, None]
    angle = 2 * math.pi * ((k1 * np.arange(LA)[None, :]) % LA) / LA
    live = k1 <= LA // 2
    first = np.concatenate([np.cos(angle) * live, -np.sin(angle) * live], axis=0)
    high, low = split_np(first)
    first = np.concatenate([high, high, low], axis=1)
    angle = 2 * math.pi * (k1 * np.arange(LB)[None, :]) / SEG
    scale = math.sqrt(1.0 / (0.375 * SEG)) * live
    twiddle = np.stack([np.cos(angle) * scale, -np.sin(angle) * scale]).astype(np.float32)
    own = LB // 2 // shards
    d = np.arange(shards)
    k2 = [own * d + e for e in range(own)] + [LB - 1 - own * d - e for e in range(own)]
    k2 = np.concatenate(k2)[None, :]
    angle = 2 * math.pi * ((np.arange(LB)[:, None] * k2) % LB) / LB
    c, s = np.cos(angle), -np.sin(angle)
    second = np.concatenate([np.concatenate([c, s], 1), np.concatenate([-s, c], 1)], 0)
    high, low = split_np(second)
    second = np.concatenate([high, high, low], axis=0)
    n = np.arange(SEG)
    window = (0.5 - 0.5 * np.cos(2 * math.pi * n / SEG)).reshape(LA, LB).astype(np.float32)
    return first, second, twiddle, window


def pack_kernel(per, mask_ref, x_ref, o_ref, a_ref, b_ref, c_ref, h_ref):
    me = lax.axis_index("tm")
    channels = GROUP * per
    rows = x_ref.shape[0] // channels
    half = rows // 2
    even = lax.rem(me, 2) == 0

    def masks(ref, at, first):
        ref[at : at + 8, :] = jnp.zeros((8, LANES), jnp.float32)
        for c in range(per):
            for s in range(2):
                value = mask_ref[first + c, s].astype(jnp.float32)
                ref[at + 2 * c + s : at + 2 * c + s + 1, :] = jnp.full((1, LANES), value)

    for ref, shift in ((a_ref, 1), (b_ref, GROUP - 1), (c_ref, 2), (o_ref, 0)):
        first = per * lax.rem(me + shift, GROUP)
        for c in range(per):
            ref[c * rows : (c + 1) * rows, :] = x_ref[pl.ds(first + c, rows, stride=channels), :]
        masks(ref, per * rows, first)
    first = per * lax.rem(me + jnp.where(even, GROUP - 1, 1), GROUP)
    start = jnp.where(even, half * channels, 0)
    for c in range(per):
        h_ref[c * half : (c + 1) * half, :] = x_ref[
            pl.ds(start + first + c, half, stride=channels), :
        ]
    masks(h_ref, per * half, first)


def spectra_kernel(
    per, shards, o_ref, a_ref, b_ref, c_ref, h_ref, f_ref, w_ref, tw_ref, win_ref, out_ref
):
    me = lax.axis_index("tm")
    even = lax.rem(me, 2) == 0
    rows = (o_ref.shape[0] - 8) // per
    half = rows // 2
    parts = 2 * (LB // 2 // shards)
    lines = 2 * parts * per
    c_index = lax.rem(me + jnp.where(even, 2, shards - 2), shards)
    after_o = jnp.where(me == shards - 1, 0.0, 1.0)
    before_o = jnp.where(me == 0, 0.0, 1.0)
    before_c = jnp.where(c_index == 0, 0.0, 1.0)
    y_index = lax.rem(me + jnp.where(even, 3, shards - 1), shards)
    before_y = jnp.where(y_index == 0, 0.0, 1.0)
    swap = (lax.broadcasted_iota(jnp.int32, (8, LANES), 0) == 0) & (
        lax.broadcasted_iota(jnp.int32, (8, LANES), 1) >= LB // 2
    )

    lane = lax.broadcasted_iota(jnp.int32, (1, LANES), 1)

    def one_channel(c, carry):
        base = pl.multiple_of(c * rows, rows)
        h_base = pl.multiple_of(c * half, half)

        def halves(ref):
            return ref[pl.ds(base, half), :], ref[pl.ds(base + half, half), :]

        def weight(ref, s, at):
            return ref[pl.ds(at + 2 * c + s, 1), :]

        mask_at, h_mask_at = per * rows, per * half
        o0, o1 = halves(o_ref)
        a0, a1 = halves(a_ref)
        b0, b1 = halves(b_ref)
        c0, c1 = halves(c_ref)
        h = h_ref[pl.ds(h_base, half), :]
        x1 = jnp.where(even, b1, h)
        y = jnp.where(even, h, a0)
        x_weight = jnp.where(even, weight(b_ref, 1, mask_at), weight(h_ref, 1, h_mask_at))
        pairs = (
            ((a0, a1, None, weight(a_ref, 0, mask_at)), (a1, o0, before_o, weight(a_ref, 1, mask_at))),
            ((o0, o1, None, weight(o_ref, 0, mask_at)), (o1, b0, after_o, weight(o_ref, 1, mask_at))),
            ((b0, b1, None, weight(b_ref, 0, mask_at)), (x1, c0, before_c, x_weight)),
            ((c0, c1, None, weight(c_ref, 0, mask_at)), (c1, y, before_y, weight(c_ref, 1, mask_at))),
        )
        peak = log_sum = None
        for pair in pairs:
            framed = []
            for head, tail, live, _ in pair:
                tail = tail * win_ref[half:, :]
                if live is not None:
                    tail = tail * live
                framed.append(jnp.concatenate([head * win_ref[:half, :], tail], axis=0))
            high, low = split(jnp.concatenate(framed, axis=1))
            mid = jnp.dot(
                f_ref[...],
                jnp.concatenate([high, low, high], axis=0),
                preferred_element_type=jnp.float32,
            )
            turned = []
            for s in range(2):
                re = mid[:ROWS, s * LB : (s + 1) * LB]
                im = mid[ROWS:, s * LB : (s + 1) * LB]
                turned.append(
                    jnp.concatenate(
                        [re * tw_ref[0] - im * tw_ref[1], re * tw_ref[1] + im * tw_ref[0]], axis=1
                    )
                )
            high, low = split(jnp.concatenate(turned, axis=0))
            out = jnp.dot(
                jnp.concatenate([high, low, high], axis=1),
                w_ref[...],
                preferred_element_type=jnp.float32,
            )
            powers = out[:, :LB] * out[:, :LB] + out[:, LB:] * out[:, LB:]
            for s in range(2):
                mine = powers[s * ROWS : (s + 1) * ROWS]
                first = jnp.where(swap, mine[LA // 2 : LA // 2 + 8], mine[:8])
                mine = jnp.concatenate([first, mine[8 : LA // 2]], axis=0)
                keep = pair[s][3]
                kept_power = keep * mine
                kept_log = keep * jnp.log(0.25 + mine)
                peak = kept_power if peak is None else jnp.maximum(peak, kept_power)
                log_sum = kept_log if log_sum is None else log_sum + kept_log
        for kind, value in enumerate((peak, log_sum)):
            turned = jnp.transpose(value)
            for i in range(parts):
                out_ref[pl.ds((kind * parts + i) * per + c, shards, stride=lines + 1), :] = turned[
                    i * shards : (i + 1) * shards
                ]
        kept = sum(w for pair in pairs for _, _, _, w in pair)
        return jnp.where(lane == c, kept, carry)

    kept = lax.fori_loop(0, per, one_channel, jnp.zeros((1, LANES), jnp.float32))
    out_ref[pl.ds(lines, shards, stride=lines + 1), :] = jnp.broadcast_to(kept, (shards, LANES))


def joined(ref, per, own, kind, op):
    parts = 2 * own
    size = parts * per
    step = 2 * size + 1
    shards = ref.shape[0] // step
    lane = lax.broadcasted_iota(jnp.int32, (GROUP * per, LANES), 1)
    back = jnp.where(lane == 0, 0, LANES - lane)
    sets = []
    for r in range(GROUP):
        total = None
        for q in range(shards // GROUP):
            at = (GROUP * q + r) * step + kind * size
            term = ref[at : at + size, :]
            total = term if total is None else op(total, term)
        sets.append(total)
    pieces = []
    for e in range(own):
        for i, mirrored in ((e, False), (own + e, True)):
            piece = jnp.concatenate([t[i * per : (i + 1) * per] for t in sets], axis=0)
            if mirrored:
                piece = jnp.take_along_axis(piece, back, axis=1)
            pieces.append(piece)
    return jnp.concatenate(pieces, axis=1)


def finish_kernel(per, own, assign_ref, z_ref, peak_ref, log_ref, part_ref):
    channels = GROUP * per
    lines = 4 * own * per
    step = lines + 1
    shards = z_ref.shape[0] // step
    lane = lax.broadcasted_iota(jnp.int32, (channels, LANES), 1)
    line = lax.broadcasted_iota(jnp.int32, (channels, LANES), 0)
    kept = jnp.zeros((channels, LANES), jnp.float32)
    for r in range(GROUP):
        row = jnp.zeros((1, LANES), jnp.float32)
        for q in range(shards // GROUP):
            at = (GROUP * q + r) * step + lines
            row = row + z_ref[at : at + 1, :]
        kept = jnp.where((line - per * r == lane) & (lane < per), row, kept)
    kept = jnp.sum(kept, axis=1, keepdims=True)
    log_mean = joined(z_ref, per, own, 1, jnp.add) / kept
    peak_ref[...] = joined(z_ref, per, own, 0, jnp.maximum)
    log_ref[...] = log_mean
    bins = log_mean.shape[1]
    block = lax.broadcasted_iota(jnp.int32, (BLOCKS, bins), 0)
    block_small = lax.broadcasted_iota(jnp.int32, (BLOCKS, LANES), 0)
    sums = jnp.zeros((BLOCKS, bins), jnp.float32)
    counts = jnp.zeros((BLOCKS, LANES), jnp.float32)
    for c in range(channels):
        sums = sums + jnp.where(block == assign_ref[c], log_mean[c : c + 1], 0.0)
        counts = counts + jnp.where(block_small == assign_ref[c], 1.0, 0.0)
    both = jnp.concatenate([sums, counts], axis=1)
    for p in range(part_ref.shape[0]):
        part_ref[p] = both


def blocks_kernel(parts_ref, out_ref):
    total = parts_ref[0]
    for p in range(1, parts_ref.shape[0]):
        total = total + parts_ref[p]
    bins = out_ref.shape[1]
    out_ref[...] = total[:, :bins] / total[:, bins : bins + 1]


VMEM = pl.BlockSpec(memory_space=pltpu.VMEM)
SMEM = pl.BlockSpec(memory_space=pltpu.SMEM)
PARAMS = pltpu.CompilerParams(vmem_limit_bytes=48 * 1024 * 1024)


def f32(*shape):
    return jax.ShapeDtypeStruct(shape, jnp.float32)


def on_device(signal, gap_mask, assignment):
    channels, local_time = signal.shape
    shards = lax.axis_size("tm")
    per = channels // GROUP
    rows = local_time // LANES
    half_bins = SEG // 2
    bins = half_bins // shards
    own = LB // 2 // shards
    lines = 4 * own * per
    first, second, twiddle, window = tables(shards)

    lined = signal.reshape(channels, rows, LANES).transpose(1, 0, 2).reshape(-1, LANES)
    size, small = per * rows + 8, per * rows // 2 + 8
    o, a, b, c, h = pl.pallas_call(
        functools.partial(pack_kernel, per),
        out_shape=[f32(size, LANES)] * 4 + [f32(small, LANES)],
        in_specs=[SMEM, VMEM],
        out_specs=[VMEM] * 5,
        compiler_params=PARAMS,
        name="pack",
    )(gap_mask, lined)

    def moved(x, by):
        return lax.ppermute(x, "tm", [(i, (i + by(i)) % shards) for i in range(shards)])

    a = moved(a, lambda i: 1)
    b = moved(b, lambda i: -1)
    c = moved(c, lambda i: 2 if i % 2 else -2)
    h = moved(h, lambda i: -3 if i % 2 else 3)

    sums = pl.pallas_call(
        functools.partial(spectra_kernel, per, shards),
        out_shape=f32(shards * (lines + 1), LANES),
        in_specs=[VMEM] * 9,
        out_specs=VMEM,
        compiler_params=PARAMS,
        cost_estimate=pl.CostEstimate(
            flops=4_000_000_000, bytes_accessed=4_000_000, transcendentals=300_000
        ),
        name="spectra",
    )(o, a, b, c, h, jnp.asarray(first), jnp.asarray(second), twiddle, window)
    sums = lax.all_to_all(sums.reshape(shards, 1, -1), "tm", 0, 0, tiled=True)
    peers = lax.axis_size(("chan", "sub"))
    peak_hold, log_mean, part = pl.pallas_call(
        functools.partial(finish_kernel, per, own),
        out_shape=[f32(channels, bins), f32(channels, bins), f32(peers, BLOCKS, bins + LANES)],
        in_specs=[SMEM, VMEM],
        out_specs=[VMEM] * 3,
        compiler_params=PARAMS,
        name="finish",
    )(assignment, sums.reshape(-1, LANES))
    part = lax.all_to_all(part, ("chan", "sub"), 0, 0, tiled=True)
    block_mean = pl.pallas_call(
        blocks_kernel,
        out_shape=f32(BLOCKS, bins),
        in_specs=[VMEM],
        out_specs=VMEM,
        compiler_params=PARAMS,
        name="blocks",
    )(part)
    return peak_hold, log_mean, block_mean


def solution(mesh):
    in_specs = (
        P(("grp", "chan", "sub"), "tm"),
        P(("grp", "chan", "sub"), "tm"),
        P(("grp", "chan", "sub")),
    )
    out_specs = (P(("grp", "chan", "sub"), "tm"), P(("grp", "chan", "sub"), "tm"), P("grp", "tm"))
    return jax.shard_map(
        on_device, mesh=mesh, in_specs=in_specs, out_specs=out_specs, check_vma=False
    )
```

```python
import functools
import math

import jax
import jax.numpy as jnp
import numpy as np
from jax import lax
from jax.experimental import pallas as pl
from jax.experimental.pallas import tpu as pltpu
from jax.sharding import PartitionSpec as P

LA = 256
LB = 128
BLOCKS = 8
SEG = LA * LB
GROUP = 4
ROWS = 144
LANES = 128


def split(x):
    high = x.astype(jnp.bfloat16)
    return high, (x - high.astype(jnp.float32)).astype(jnp.bfloat16)


def split_np(x):
    high = x.astype(np.float32).astype(jnp.bfloat16)
    low = (x - high.astype(np.float64)).astype(np.float32).astype(jnp.bfloat16)
    return high, low


@functools.lru_cache
def tables(shards):
    k1 = np.arange(ROWS)[:, None]
    angle = 2 * math.pi * ((k1 * np.arange(LA)[None, :]) % LA) / LA
    live = k1 <= LA // 2
    first = np.concatenate([np.cos(angle) * live, -np.sin(angle) * live], axis=0)
    high, low = split_np(first)
    first = np.concatenate([high, high, low], axis=1)
    angle = 2 * math.pi * (k1 * np.arange(LB)[None, :]) / SEG
    scale = math.sqrt(1.0 / (0.375 * SEG)) * live
    twiddle = np.stack([np.cos(angle) * scale, -np.sin(angle) * scale]).astype(np.float32)
    own = LB // 2 // shards
    d = np.arange(shards).reshape(-1, GROUP).T
    k2 = [own * d + e for e in range(own)] + [LB - 1 - own * d - e for e in range(own)]
    k2 = np.stack(k2, axis=1).reshape(1, -1)
    angle = 2 * math.pi * ((np.arange(LB)[:, None] * k2) % LB) / LB
    c, s = np.cos(angle), -np.sin(angle)
    second = np.concatenate([np.concatenate([c, s], 1), np.concatenate([-s, c], 1)], 0)
    high, low = split_np(second)
    second = np.concatenate([high, high, low], axis=0)
    n = np.arange(SEG)
    window = (0.5 - 0.5 * np.cos(2 * math.pi * n / SEG)).reshape(LA, LB).astype(np.float32)
    return first, second, np.concatenate([*twiddle, window], axis=0)


def pack_kernel(per, mask_ref, x_ref, o_ref, a_ref, b_ref, c_ref, h_ref):
    me = lax.axis_index("tm")
    channels = GROUP * per
    rows = x_ref.shape[0] // channels
    half = rows // 2
    even = lax.rem(me, 2) == 0

    def masks(ref, at, first):
        ref[at : at + 8, :] = jnp.zeros((8, LANES), jnp.float32)
        for c in range(per):
            for s in range(2):
                value = mask_ref[s, first + c].astype(jnp.float32)
                ref[at + 2 * c + s : at + 2 * c + s + 1, :] = jnp.full((1, LANES), value)

    for ref, shift in ((c_ref, 2), (a_ref, 1), (b_ref, GROUP - 1), (o_ref, 0)):
        first = per * lax.rem(me + shift, GROUP)
        for c in range(per):
            ref[c * rows : (c + 1) * rows, :] = x_ref[pl.ds(first + c, rows, stride=channels), :]
        masks(ref, per * rows, first)
    first = per * lax.rem(me + 2, GROUP)
    start = jnp.where(even, half * channels, 0)
    for c in range(per):
        h_ref[c * half : (c + 1) * half, :] = x_ref[
            pl.ds(start + first + c, half, stride=channels), :
        ]
    masks(h_ref, per * half, first)


def spectra_kernel(per, shards, o_ref, a_ref, b_ref, c_ref, h_ref, f_ref, w_ref, t_ref, out_ref):
    me = lax.axis_index("tm")
    even = lax.rem(me, 2) == 0
    rows = (o_ref.shape[0] - 8) // per
    half = rows // 2
    sets = shards // GROUP
    parts = LB // sets
    lines = 2 * parts * per
    starts_a = jnp.where(me == 1, 0.0, 1.0)
    starts_o = jnp.where(me == 0, 0.0, 1.0)
    starts_b = jnp.where(me == shards - 1, 0.0, 1.0)
    starts_y = jnp.where(me == shards - 2, 0.0, 1.0)
    lane = lax.broadcasted_iota(jnp.int32, (1, LANES), 1)
    swap = (lax.broadcasted_iota(jnp.int32, (8, LANES), 0) == 0) & (
        lax.rem(lax.broadcasted_iota(jnp.int32, (8, LANES), 1), parts // GROUP * sets)
        >= parts // GROUP // 2 * sets
    )

    def one_channel(c, carry):
        base = pl.multiple_of(c * rows, rows)

        def halves(ref):
            return ref[pl.ds(base, half), :], ref[pl.ds(base + half, half), :]

        def weight(ref, s, at=per * rows):
            return ref[pl.ds(at + 2 * c + s, 1), :]

        o0, o1 = halves(o_ref)
        a0, a1 = halves(a_ref)
        b0, b1 = halves(b_ref)
        c0, c1 = halves(c_ref)
        h = h_ref[pl.ds(pl.multiple_of(c * half, half), half), :]
        x = jnp.where(even, h, c1)
        y = jnp.where(even, c0, h)
        x_weight = jnp.where(even, weight(h_ref, 1, per * half), weight(c_ref, 1))
        pairs = (
            ((o0, o1, None, weight(o_ref, 0)), (o1, b0, starts_b, weight(o_ref, 1))),
            ((a0, a1, None, weight(a_ref, 0)), (a1, o0, starts_o, weight(a_ref, 1))),
            ((b0, b1, None, weight(b_ref, 0)), (b1, y, starts_y, weight(b_ref, 1))),
            ((c0, c1, None, weight(c_ref, 0)), (x, a0, starts_a, x_weight)),
        )
        window = t_ref[2 * ROWS :, :]
        peak = log_sum = None
        for pair in pairs:
            framed = []
            for head, tail, live, _ in pair:
                tail = tail * window[half:]
                if live is not None:
                    tail = tail * live
                framed.append(jnp.concatenate([head * window[:half], tail], axis=0))
            high, low = split(jnp.concatenate(framed, axis=1))
            mid = jnp.dot(
                f_ref[...],
                jnp.concatenate([high, low, high], axis=0),
                preferred_element_type=jnp.float32,
            )
            cosine, sine = t_ref[:ROWS, :], t_ref[ROWS : 2 * ROWS, :]
            turned = []
            for s in range(2):
                re = mid[:ROWS, s * LB : (s + 1) * LB]
                im = mid[ROWS:, s * LB : (s + 1) * LB]
                turned.append(
                    jnp.concatenate([re * cosine - im * sine, re * sine + im * cosine], axis=1)
                )
            high, low = split(jnp.concatenate(turned, axis=0))
            out = jnp.dot(
                jnp.concatenate([high, low, high], axis=1),
                w_ref[...],
                preferred_element_type=jnp.float32,
            )
            powers = out[:, :LB] * out[:, :LB] + out[:, LB:] * out[:, LB:]
            for s in range(2):
                mine = powers[s * ROWS : (s + 1) * ROWS]
                first = jnp.where(swap, mine[LA // 2 : LA // 2 + 8], mine[:8])
                mine = jnp.concatenate([first, mine[8 : LA // 2]], axis=0)
                keep = pair[s][3]
                kept_power = keep * mine
                kept_log = keep * jnp.log(0.25 + mine)
                peak = kept_power if peak is None else jnp.maximum(peak, kept_power)
                log_sum = kept_log if log_sum is None else log_sum + kept_log
        for kind, value in enumerate((peak, log_sum)):
            turned = jnp.transpose(value)
            for i in range(parts):
                out_ref[pl.ds((kind * parts + i) * per + c, sets, stride=lines + 1), :] = turned[
                    i * sets : (i + 1) * sets
                ]
        kept = sum(w for pair in pairs for _, _, _, w in pair)
        return jnp.where(lane == c, kept, carry)

    kept = lax.fori_loop(0, per, one_channel, jnp.zeros((1, LANES), jnp.float32))
    out_ref[pl.ds(lines, sets, stride=lines + 1), :] = jnp.broadcast_to(kept, (sets, LANES))


def join_kernel(per, sets, peers, assign_ref, z_ref, out_ref):
    lines = z_ref.shape[0] // sets
    size = (lines - 1) // 2 // GROUP
    first = per * lax.rem(lax.axis_index("tm"), GROUP)
    lane = lax.broadcasted_iota(jnp.int32, (size, LANES), 1)
    line = lax.broadcasted_iota(jnp.int32, (size, LANES), 0)

    def joined(at, count, op):
        total = z_ref[at : at + count, :]
        for q in range(1, sets):
            total = op(total, z_ref[q * lines + at : q * lines + at + count, :])
        return total

    kept = joined(lines - 1, 1, jnp.add)
    kept = jnp.sum(jnp.where(lane == lax.rem(line, per), kept, 0.0), axis=1, keepdims=True)
    ids = [jnp.full((1, LANES), assign_ref[first + c].astype(jnp.float32)) for c in range(per)]
    ids = jnp.concatenate(ids, axis=0)
    step = 2 * size + per
    for r in range(GROUP):
        peak = joined(r * size, size, jnp.maximum)
        log_mean = joined((GROUP + r) * size, size, jnp.add) / kept
        for p in range(peers):
            at = (r * peers + p) * step
            out_ref[at : at + size, :] = peak
            out_ref[at + size : at + 2 * size, :] = log_mean
            out_ref[at + 2 * size : at + step, :] = ids


def finish_kernel(per, peers, z_ref, peak_ref, log_ref, block_ref):
    me = lax.axis_index(("chan", "sub"))
    step = z_ref.shape[0] // (GROUP * peers)
    size = (step - per) // 2
    parts = size // per
    own = parts // 2
    lane = lax.broadcasted_iota(jnp.int32, (GROUP * per, LANES), 1)
    back = jnp.where(lane == 0, 0, LANES - lane)

    def in_order(pieces):
        out = []
        for e in range(own):
            out.append(pieces[e])
            out.append(jnp.take_along_axis(pieces[own + e], back, axis=1))
        return jnp.concatenate(out, axis=1)

    for kind, ref in enumerate((peak_ref, log_ref)):
        mine = []
        for r in range(GROUP):
            value = None
            for p in range(peers):
                at = (r * peers + p) * step + kind * size
                term = z_ref[at : at + size, :]
                value = term if value is None else jnp.where(me == p, term, value)
            mine.append(value)
        ref[...] = in_order(
            [
                jnp.concatenate([m[i * per : (i + 1) * per] for m in mine], axis=0)
                for i in range(parts)
            ]
        )
    block = lax.broadcasted_iota(jnp.int32, (BLOCKS, LANES), 0).astype(jnp.float32)
    sums = [jnp.zeros((BLOCKS, LANES), jnp.float32)] * parts
    counts = jnp.zeros((BLOCKS, LANES), jnp.float32)
    for s in range(GROUP * peers):
        at = s * step
        for c in range(per):
            inside = block == z_ref[at + 2 * size + c : at + 2 * size + c + 1, :]
            counts = counts + jnp.where(inside, 1.0, 0.0)
            for i in range(parts):
                row = at + size + i * per + c
                sums[i] = sums[i] + jnp.where(inside, z_ref[row : row + 1, :], 0.0)
    block_ref[...] = in_order([total / counts for total in sums])


VMEM = pl.BlockSpec(memory_space=pltpu.VMEM)
SMEM = pl.BlockSpec(memory_space=pltpu.SMEM)
PARAMS = pltpu.CompilerParams(vmem_limit_bytes=48 * 1024 * 1024)


def f32(*shape):
    return jax.ShapeDtypeStruct(shape, jnp.float32)


def on_device(signal, gap_mask, assignment):
    channels, local_time = signal.shape
    shards = lax.axis_size("tm")
    peers = lax.axis_size(("chan", "sub"))
    sets = shards // GROUP
    per = channels // GROUP
    rows = local_time // LANES
    bins = SEG // 2 // shards
    size = bins // LANES * per
    first, second, tables_f32 = tables(shards)

    lined = signal.reshape(channels, rows, LANES).transpose(1, 0, 2).reshape(-1, LANES)
    whole, small = per * rows + 8, per * rows // 2 + 8
    o, a, b, c, h = pl.pallas_call(
        functools.partial(pack_kernel, per),
        out_shape=[f32(whole, LANES)] * 4 + [f32(small, LANES)],
        in_specs=[SMEM, VMEM],
        out_specs=[VMEM] * 5,
        compiler_params=PARAMS,
        name="pack",
    )(gap_mask.T, lined)

    def moved(x, by):
        return lax.ppermute(x, "tm", [(i, (i + by(i)) % shards) for i in range(shards)])

    c = moved(c, lambda i: 2 if i % 2 else -2)
    h = moved(h, lambda i: -2 if i % 2 else 2)
    a = moved(a, lambda i: 1)
    b = moved(b, lambda i: -1)

    lines = 2 * GROUP * size + 1
    sums = pl.pallas_call(
        functools.partial(spectra_kernel, per, shards),
        out_shape=f32(sets * lines, LANES),
        in_specs=[VMEM] * 8,
        out_specs=VMEM,
        compiler_params=PARAMS,
        cost_estimate=pl.CostEstimate(
            flops=4_000_000_000, bytes_accessed=4_000_000, transcendentals=300_000
        ),
        name="spectra",
    )(o, a, b, c, h, jnp.asarray(first), jnp.asarray(second), tables_f32)
    sums = lax.all_to_all(
        sums.reshape(sets, 1, -1),
        "tm",
        0,
        0,
        tiled=True,
        axis_index_groups=[[GROUP * q + r for q in range(sets)] for r in range(GROUP)],
    )
    step = 2 * size + per
    near = GROUP * peers
    joined = pl.pallas_call(
        functools.partial(join_kernel, per, sets, peers),
        out_shape=f32(near * step, LANES),
        in_specs=[SMEM, VMEM],
        out_specs=VMEM,
        compiler_params=PARAMS,
        name="join",
    )(assignment, sums.reshape(-1, LANES))
    joined = lax.all_to_all(
        joined.reshape(near, 1, -1),
        ("tm", "chan", "sub"),
        0,
        0,
        tiled=True,
        axis_index_groups=[[near * q + s for s in range(near)] for q in range(sets)],
    )
    return pl.pallas_call(
        functools.partial(finish_kernel, per, peers),
        out_shape=[f32(channels, bins), f32(channels, bins), f32(BLOCKS, bins)],
        in_specs=[VMEM],
        out_specs=[VMEM] * 3,
        compiler_params=PARAMS,
        name="finish",
    )(joined.reshape(-1, LANES))


def solution(mesh):
    in_specs = (
        P(("grp", "chan", "sub"), "tm"),
        P(("grp", "chan", "sub"), "tm"),
        P(("grp", "chan", "sub")),
    )
    out_specs = (P(("grp", "chan", "sub"), "tm"), P(("grp", "chan", "sub"), "tm"), P("grp", "tm"))
    return jax.shard_map(
        on_device, mesh=mesh, in_specs=in_specs, out_specs=out_specs, check_vma=False
    )
```

```python
import functools
import math

import jax
import jax.numpy as jnp
import numpy as np
from jax import lax
from jax.experimental import pallas as pl
from jax.experimental.pallas import tpu as pltpu
from jax.sharding import PartitionSpec as P

LA = 256
LB = 128
BLOCKS = 8
SEG = LA * LB
GROUP = 4
ROWS = 144
LANES = 128


def split(x):
    high = x.astype(jnp.bfloat16)
    return high, (x - high.astype(jnp.float32)).astype(jnp.bfloat16)


def owners(shards, role):
    return [
        GROUP * (2 * m + (role + r) % 2) + r
        for m in range(shards // GROUP // 2)
        for r in range(GROUP)
    ]


@functools.lru_cache
def tables(shards):
    k1 = np.arange(ROWS)[:, None]
    angle = 2 * math.pi * ((k1 * np.arange(LA)[None, :]) % LA) / LA
    live = k1 <= LA // 2
    first = np.concatenate([np.cos(angle) * live, -np.sin(angle) * live], axis=0)
    angle = 2 * math.pi * (k1 * np.arange(LB)[None, :]) / SEG
    scale = math.sqrt(1.0 / (0.375 * SEG)) * live
    twiddle = np.cos(angle) * scale, -np.sin(angle) * scale
    own = LB // 2 // shards
    roles = [owners(shards, role) for role in range(2)]
    k2 = [
        k
        for d in map(np.array, roles)
        for k in [own * d + e for e in range(own)] + [LB - 1 - own * d - e for e in range(own)]
    ]
    k2 = np.concatenate(k2)[None, :]
    angle = 2 * math.pi * ((np.arange(LB)[:, None] * k2) % LB) / LB
    c, s = np.cos(angle), -np.sin(angle)
    second = np.concatenate([np.concatenate([c, s], 1), np.concatenate([-s, c], 1)], 0)
    n = np.arange(SEG)
    window = (0.5 - 0.5 * np.cos(2 * math.pi * n / SEG)).reshape(LA, LB)
    halves = [x[:, at : at + LANES] for x in (first, second) for at in (0, LANES)]
    return np.concatenate([*twiddle, window, *halves], axis=0).astype(np.float32)


def pack_kernel(per, mask_ref, assign_ref, x_ref, *refs):
    o_ref, a_ref, b_ref, c_ref, h_ref, ids_ref = refs
    me = lax.axis_index("tm")
    channels = GROUP * per
    rows = x_ref.shape[0] // channels
    half = rows // 2
    even = lax.rem(me, 2) == 0
    for c in range(channels):
        ids_ref[c : c + 1, :] = jnp.full((1, LANES), assign_ref[c].astype(jnp.float32))

    def masks(ref, at, first):
        ref[at : at + 8, :] = jnp.zeros((8, LANES), jnp.float32)
        for c in range(per):
            for s in range(2):
                value = mask_ref[s, first + c].astype(jnp.float32)
                ref[at + 2 * c + s : at + 2 * c + s + 1, :] = jnp.full((1, LANES), value)

    for ref, shift in ((c_ref, 2), (a_ref, 1), (b_ref, GROUP - 1), (o_ref, 0)):
        first = per * lax.rem(me + shift, GROUP)
        for c in range(per):
            ref[c * rows : (c + 1) * rows, :] = x_ref[pl.ds(first + c, rows, stride=channels), :]
        masks(ref, per * rows, first)
    first = per * lax.rem(me + 2, GROUP)
    start = jnp.where(even, half * channels, 0)
    for c in range(per):
        h_ref[c * half : (c + 1) * half, :] = x_ref[
            pl.ds(start + first + c, half, stride=channels), :
        ]
    masks(h_ref, per * half, first)


def spectra_kernel(per, shards, *refs):
    o_ref, a_ref, b_ref, c_ref, h_ref, t_ref, keep_ref, send_ref, f_ref, w_ref = refs
    at = 2 * ROWS + LA
    side = t_ref[at : at + 2 * ROWS, :], t_ref[at + 2 * ROWS : at + 4 * ROWS, :]
    high, low = split(jnp.concatenate(side, axis=1))
    f_ref[...] = jnp.concatenate([high, high, low], axis=1)
    at += 4 * ROWS
    side = t_ref[at : at + 2 * LB, :], t_ref[at + 2 * LB :, :]
    high, low = split(jnp.concatenate(side, axis=1))
    w_ref[...] = jnp.concatenate([high, high, low], axis=0)
    me = lax.axis_index("tm")
    even = lax.rem(me, 2) == 0
    role = lax.rem(me // GROUP + lax.rem(me, GROUP), 2)
    rows = (o_ref.shape[0] - 8) // per
    half = rows // 2
    dests = shards // 2
    parts = LB // shards
    lines = 2 * parts * per
    starts_a = jnp.where(me == 1, 0.0, 1.0)
    starts_o = jnp.where(me == 0, 0.0, 1.0)
    starts_b = jnp.where(me == shards - 1, 0.0, 1.0)
    starts_y = jnp.where(me == shards - 2, 0.0, 1.0)
    lane = lax.broadcasted_iota(jnp.int32, (1, LANES), 1)
    swap = (lax.broadcasted_iota(jnp.int32, (8, LANES), 0) == 0) & (
        lax.rem(lax.broadcasted_iota(jnp.int32, (8, LANES), 1), LB // 2) >= LB // 4
    )

    def one_channel(c, carry):
        base = pl.multiple_of(c * rows, rows)

        def halves(ref):
            return ref[pl.ds(base, half), :], ref[pl.ds(base + half, half), :]

        def weight(ref, s, at=per * rows):
            return ref[pl.ds(at + 2 * c + s, 1), :]

        o0, o1 = halves(o_ref)
        a0, a1 = halves(a_ref)
        b0, b1 = halves(b_ref)
        c0, c1 = halves(c_ref)
        h = h_ref[pl.ds(pl.multiple_of(c * half, half), half), :]
        x = jnp.where(even, h, c1)
        y = jnp.where(even, c0, h)
        x_weight = jnp.where(even, weight(h_ref, 1, per * half), weight(c_ref, 1))
        pairs = (
            ((o0, o1, None, weight(o_ref, 0)), (o1, b0, starts_b, weight(o_ref, 1))),
            ((a0, a1, None, weight(a_ref, 0)), (a1, o0, starts_o, weight(a_ref, 1))),
            ((b0, b1, None, weight(b_ref, 0)), (b1, y, starts_y, weight(b_ref, 1))),
            ((c0, c1, None, weight(c_ref, 0)), (x, a0, starts_a, x_weight)),
        )
        window = t_ref[2 * ROWS : 2 * ROWS + LA, :]
        peak = log_sum = None
        for pair in pairs:
            framed = []
            for head, tail, live, _ in pair:
                tail = tail * window[half:]
                if live is not None:
                    tail = tail * live
                framed.append(jnp.concatenate([head * window[:half], tail], axis=0))
            high, low = split(jnp.concatenate(framed, axis=1))
            mid = jnp.dot(
                f_ref[...],
                jnp.concatenate([high, low, high], axis=0),
                preferred_element_type=jnp.float32,
            )
            cosine, sine = t_ref[:ROWS, :], t_ref[ROWS : 2 * ROWS, :]
            turned = []
            for s in range(2):
                re = mid[:ROWS, s * LB : (s + 1) * LB]
                im = mid[ROWS:, s * LB : (s + 1) * LB]
                turned.append(
                    jnp.concatenate([re * cosine - im * sine, re * sine + im * cosine], axis=1)
                )
            high, low = split(jnp.concatenate(turned, axis=0))
            out = jnp.dot(
                jnp.concatenate([high, low, high], axis=1),
                w_ref[...],
                preferred_element_type=jnp.float32,
            )
            powers = out[:, :LB] * out[:, :LB] + out[:, LB:] * out[:, LB:]
            for s in range(2):
                mine = powers[s * ROWS : (s + 1) * ROWS]
                first = jnp.where(swap, mine[LA // 2 : LA // 2 + 8], mine[:8])
                mine = jnp.concatenate([first, mine[8 : LA // 2]], axis=0)
                keep = pair[s][3]
                kept_power = keep * mine
                kept_log = keep * jnp.log(0.25 + mine)
                peak = kept_power if peak is None else jnp.maximum(peak, kept_power)
                log_sum = kept_log if log_sum is None else log_sum + kept_log
        for kind, value in enumerate((peak, log_sum)):
            turned = jnp.transpose(value)
            for ref, mine in ((keep_ref, 0), (send_ref, 1)):
                chosen = jnp.where(role == mine, turned[: LB // 2], turned[LB // 2 :])
                for i in range(parts):
                    at = (kind * parts + i) * per + c
                    ref[pl.ds(at, dests, stride=lines + 1), :] = chosen[
                        i * dests : (i + 1) * dests
                    ]
        kept = sum(w for pair in pairs for _, _, _, w in pair)
        return jnp.where(lane == c, kept, carry)

    kept = lax.fori_loop(0, per, one_channel, jnp.zeros((1, LANES), jnp.float32))
    for ref in (keep_ref, send_ref):
        ref[pl.ds(lines, dests, stride=lines + 1), :] = jnp.broadcast_to(kept, (dests, LANES))


def join_kernel(lines, mine_ref, other_ref, out_ref):
    mine, other = mine_ref[...], other_ref[...]
    line = lax.rem(lax.broadcasted_iota(jnp.int32, mine.shape, 0), lines)
    out_ref[...] = jnp.where(line < lines // 2, jnp.maximum(mine, other), mine + other)


def finish_kernel(per, ids_ref, z_ref, peak_ref, log_ref, part_ref):
    channels, bins = log_ref.shape
    parts = bins // LANES
    own = parts // 2
    size = parts * per
    step = 2 * size + 1
    sources = z_ref.shape[0] // step
    lane = lax.broadcasted_iota(jnp.int32, (channels, LANES), 1)
    line = lax.broadcasted_iota(jnp.int32, (channels, LANES), 0)
    back = jnp.where(lane == 0, 0, LANES - lane)

    def joined(r, at, count, op):
        total = None
        for s in range(r, sources, GROUP):
            term = z_ref[s * step + at : s * step + at + count, :]
            total = term if total is None else op(total, term)
        return total

    def in_order(kind, op):
        sets = [joined(r, kind * size, size, op) for r in range(GROUP)]
        pieces = []
        for e in range(own):
            for i, mirrored in ((e, False), (own + e, True)):
                piece = jnp.concatenate([t[i * per : (i + 1) * per] for t in sets], axis=0)
                if mirrored:
                    piece = jnp.take_along_axis(piece, back, axis=1)
                pieces.append(piece)
        return jnp.concatenate(pieces, axis=1)

    kept = jnp.zeros((channels, LANES), jnp.float32)
    for r in range(GROUP):
        row = joined(r, 2 * size, 1, jnp.add)
        kept = jnp.where((line - per * r == lane) & (lane < per), row, kept)
    log_mean = in_order(1, jnp.add) / jnp.sum(kept, axis=1, keepdims=True)
    log_ref[...] = log_mean
    peak_ref[...] = in_order(0, jnp.maximum)
    block = lax.broadcasted_iota(jnp.int32, (BLOCKS, LANES), 0).astype(jnp.float32)
    inside = [block == ids_ref[c : c + 1, :] for c in range(channels)]
    for i in range(parts + 1):
        total = jnp.zeros((BLOCKS, LANES), jnp.float32)
        for c in range(channels):
            term = log_mean[c : c + 1, i * LANES : (i + 1) * LANES] if i < parts else 1.0
            total = total + jnp.where(inside[c], term, 0.0)
        for p in range(part_ref.shape[0]):
            part_ref[p, i * BLOCKS : (i + 1) * BLOCKS, :] = total


def blocks_kernel(parts_ref, out_ref):
    total = parts_ref[0]
    for p in range(1, parts_ref.shape[0]):
        total = total + parts_ref[p]
    counts = total[-BLOCKS:]
    for i in range(out_ref.shape[1] // LANES):
        out_ref[:, i * LANES : (i + 1) * LANES] = total[i * BLOCKS : (i + 1) * BLOCKS] / counts


VMEM = pl.BlockSpec(memory_space=pltpu.VMEM)
SMEM = pl.BlockSpec(memory_space=pltpu.SMEM)
PARAMS = pltpu.CompilerParams(vmem_limit_bytes=48 * 1024 * 1024)


def f32(*shape):
    return jax.ShapeDtypeStruct(shape, jnp.float32)


def on_device(signal, gap_mask, assignment):
    channels, local_time = signal.shape
    shards = lax.axis_size("tm")
    per = channels // GROUP
    rows = local_time // LANES
    bins = SEG // 2 // shards

    lined = signal.reshape(channels, rows, LANES).transpose(1, 0, 2).reshape(-1, LANES)
    whole, small = per * rows + 8, per * rows // 2 + 8
    o, a, b, c, h, ids = pl.pallas_call(
        functools.partial(pack_kernel, per),
        out_shape=[f32(whole, LANES)] * 4 + [f32(small, LANES), f32(channels, LANES)],
        in_specs=[SMEM, SMEM, VMEM],
        out_specs=[VMEM] * 6,
        compiler_params=PARAMS,
        name="pack",
    )(gap_mask.T, assignment, lined)

    def moved(x, by):
        return lax.ppermute(x, "tm", [(i, (i + by(i)) % shards) for i in range(shards)])

    a = moved(a, lambda i: 1)
    b = moved(b, lambda i: -1)
    c = moved(c, lambda i: 2 if i % 2 else -2)
    h = moved(h, lambda i: -2 if i % 2 else 2)

    dests = shards // 2
    lines = 2 * (bins // LANES) * per + 1
    keep, send = pl.pallas_call(
        functools.partial(spectra_kernel, per, shards),
        out_shape=[f32(dests * lines, LANES)] * 2,
        in_specs=[VMEM] * 6,
        out_specs=[VMEM] * 2,
        scratch_shapes=[
            pltpu.VMEM((2 * ROWS, 3 * LA), jnp.bfloat16),
            pltpu.VMEM((6 * LB, 2 * LB), jnp.bfloat16),
        ],
        compiler_params=PARAMS,
        cost_estimate=pl.CostEstimate(
            flops=4_000_000_000, bytes_accessed=4_000_000, transcendentals=300_000
        ),
        name="spectra",
    )(o, a, b, c, h, tables(shards))
    roles = [owners(shards, role) for role in range(2)]
    other = moved(send, lambda i: GROUP if i in roles[0] else -GROUP)
    sums = pl.pallas_call(
        functools.partial(join_kernel, lines),
        out_shape=f32(dests * lines, LANES),
        in_specs=[VMEM] * 2,
        out_specs=VMEM,
        compiler_params=PARAMS,
        name="join",
    )(keep, other)
    sums = lax.all_to_all(
        sums.reshape(dests, 1, -1), "tm", 0, 0, tiled=True, axis_index_groups=roles
    )
    peers = lax.axis_size(("chan", "sub"))
    peak_hold, log_mean, part = pl.pallas_call(
        functools.partial(finish_kernel, per),
        out_shape=[
            f32(channels, bins),
            f32(channels, bins),
            f32(peers, (bins // LANES + 1) * BLOCKS, LANES),
        ],
        in_specs=[VMEM] * 2,
        out_specs=[VMEM] * 3,
        compiler_params=PARAMS,
        name="finish",
    )(ids, sums.reshape(-1, LANES))
    part = lax.all_to_all(part, ("chan", "sub"), 0, 0, tiled=True)
    block_mean = pl.pallas_call(
        blocks_kernel,
        out_shape=f32(BLOCKS, bins),
        in_specs=[VMEM],
        out_specs=VMEM,
        compiler_params=PARAMS,
        name="blocks",
    )(part)
    return peak_hold, log_mean, block_mean


def solution(mesh):
    in_specs = (
        P(("grp", "chan", "sub"), "tm"),
        P(("grp", "chan", "sub"), "tm"),
        P(("grp", "chan", "sub")),
    )
    out_specs = (P(("grp", "chan", "sub"), "tm"), P(("grp", "chan", "sub"), "tm"), P("grp", "tm"))
    return jax.shard_map(
        on_device, mesh=mesh, in_specs=in_specs, out_specs=out_specs, check_vma=False
    )
```

```python
import functools
import math

import jax
import jax.numpy as jnp
import numpy as np
from jax import lax
from jax.experimental import pallas as pl
from jax.experimental.pallas import tpu as pltpu
from jax.sharding import PartitionSpec as P

LA = 256
LB = 128
BLOCKS = 8
SEG = LA * LB
GROUP = 8
REACH = GROUP // 2
ROWS = 144
LANES = 128


def split(x):
    high = x.astype(jnp.bfloat16)
    return high, (x - high.astype(jnp.float32)).astype(jnp.bfloat16)


@functools.lru_cache
def tables(shards):
    k1 = np.arange(ROWS)[:, None]
    angle = 2 * math.pi * ((k1 * np.arange(LA)[None, :]) % LA) / LA
    live = k1 <= LA // 2
    first = np.concatenate([np.cos(angle) * live, -np.sin(angle) * live], axis=0)
    angle = 2 * math.pi * (k1 * np.arange(LB)[None, :]) / SEG
    scale = math.sqrt(1.0 / (0.375 * SEG)) * live
    twiddle = np.cos(angle) * scale, -np.sin(angle) * scale
    own = LB // 2 // shards
    d = np.arange(shards)
    k2 = [own * d + e for e in range(own)] + [LB - 1 - own * d - e for e in range(own)]
    k2 = np.concatenate(k2)[None, :]
    angle = 2 * math.pi * ((np.arange(LB)[:, None] * k2) % LB) / LB
    c, s = np.cos(angle), -np.sin(angle)
    second = np.concatenate([np.concatenate([c, s], 1), np.concatenate([-s, c], 1)], 0)
    n = np.arange(SEG)
    window = (0.5 - 0.5 * np.cos(2 * math.pi * n / SEG)).reshape(LA, LB)
    halves = [x[:, at : at + LANES] for x in (first, second) for at in (0, LANES)]
    return np.concatenate([*twiddle, window, *halves], axis=0).astype(np.float32)


def pack_kernel(mask_ref, assign_ref, x_ref, ids_ref, *refs):
    *whole_refs, h_ref = refs
    me = lax.axis_index("tm")
    rows = x_ref.shape[0] // GROUP
    half = rows // 2
    even = lax.rem(me, 2) == 0
    for c in range(GROUP):
        ids_ref[c : c + 1, :] = jnp.full((1, LANES), assign_ref[c].astype(jnp.float32))

    def masks(ref, at, channel):
        ref[at : at + 8, :] = jnp.zeros((8, LANES), jnp.float32)
        for s in range(2):
            value = mask_ref[s, channel].astype(jnp.float32)
            ref[at + s : at + s + 1, :] = jnp.full((1, LANES), value)

    for shift, ref in zip(range(1 - REACH, REACH + 1), whole_refs):
        channel = lax.rem(me + shift + GROUP, GROUP)
        ref[:rows, :] = x_ref[pl.ds(channel, rows, stride=GROUP), :]
        masks(ref, rows, channel)
    channel = lax.rem(me + REACH, GROUP)
    start = jnp.where(even, half * GROUP, 0)
    h_ref[:half, :] = x_ref[pl.ds(start + channel, half, stride=GROUP), :]
    masks(h_ref, half, channel)


def spectra_kernel(shards, *refs):
    *near_refs, c_ref, h_ref, t_ref, out_ref, f_ref, w_ref = refs
    at = 2 * ROWS + LA
    side = t_ref[at : at + 2 * ROWS, :], t_ref[at + 2 * ROWS : at + 4 * ROWS, :]
    high, low = split(jnp.concatenate(side, axis=1))
    f_ref[...] = jnp.concatenate([high, high, low], axis=1)
    at += 4 * ROWS
    side = t_ref[at : at + 2 * LB, :], t_ref[at + 2 * LB :, :]
    high, low = split(jnp.concatenate(side, axis=1))
    w_ref[...] = jnp.concatenate([high, high, low], axis=0)
    me = lax.axis_index("tm")
    even = lax.rem(me, 2) == 0
    rows = c_ref.shape[0] - 8
    half = rows // 2
    parts = LB // shards
    lines = 2 * parts
    swap = (lax.broadcasted_iota(jnp.int32, (8, LANES), 0) == 0) & (
        lax.broadcasted_iota(jnp.int32, (8, LANES), 1) >= LB // 2
    )

    def head(ref):
        return lambda: ref[:half, :]

    def tail(ref):
        return lambda: ref[half:rows, :]

    def weight(ref, s, at=rows):
        return ref[at + s : at + s + 1, :]

    def either(a, b):
        return lambda: jnp.where(even, a(), b())

    def live(ahead):
        return jnp.where(lax.rem(me + ahead + shards, shards) == 0, 0.0, 1.0)

    first = 1 - REACH
    segments = [(head(c_ref), tail(c_ref), None, weight(c_ref, 0))]
    x_weight = jnp.where(even, weight(h_ref, 1, half), weight(c_ref, 1))
    segments.append((either(head(h_ref), tail(c_ref)), head(near_refs[0]), live(first), x_weight))
    for i, ref in enumerate(near_refs):
        segments.append((head(ref), tail(ref), None, weight(ref, 0)))
        following = either(head(c_ref), head(h_ref))
        if i + 1 < len(near_refs):
            following = head(near_refs[i + 1])
        segments.append((tail(ref), following, live(first + i + 1), weight(ref, 1)))

    window = t_ref[2 * ROWS : 2 * ROWS + LA, :]
    peak = log_sum = kept = None
    for at in range(0, len(segments), 2):
        pair = segments[at : at + 2]
        framed = []
        for left, right, alive, _ in pair:
            right = right() * window[half:]
            if alive is not None:
                right = right * alive
            framed.append(jnp.concatenate([left() * window[:half], right], axis=0))
        high, low = split(jnp.concatenate(framed, axis=1))
        mid = jnp.dot(
            f_ref[...],
            jnp.concatenate([high, low, high], axis=0),
            preferred_element_type=jnp.float32,
        )
        cosine, sine = t_ref[:ROWS, :], t_ref[ROWS : 2 * ROWS, :]
        turned = []
        for s in range(2):
            re = mid[:ROWS, s * LB : (s + 1) * LB]
            im = mid[ROWS:, s * LB : (s + 1) * LB]
            turned.append(
                jnp.concatenate([re * cosine - im * sine, re * sine + im * cosine], axis=1)
            )
        high, low = split(jnp.concatenate(turned, axis=0))
        out = jnp.dot(
            jnp.concatenate([high, low, high], axis=1),
            w_ref[...],
            preferred_element_type=jnp.float32,
        )
        powers = out[:, :LB] * out[:, :LB] + out[:, LB:] * out[:, LB:]
        for s in range(2):
            mine = powers[s * ROWS : (s + 1) * ROWS]
            top = jnp.where(swap, mine[LA // 2 : LA // 2 + 8], mine[:8])
            mine = jnp.concatenate([top, mine[8 : LA // 2]], axis=0)
            keep = pair[s][3]
            kept_power = keep * mine
            kept_log = keep * jnp.log(0.25 + mine)
            peak = kept_power if peak is None else jnp.maximum(peak, kept_power)
            log_sum = kept_log if log_sum is None else log_sum + kept_log
            kept = keep if kept is None else kept + keep
    for kind, value in enumerate((peak, log_sum)):
        turned = jnp.transpose(value)
        for i in range(parts):
            out_ref[pl.ds(kind * parts + i, shards, stride=lines + 1), :] = turned[
                i * shards : (i + 1) * shards
            ]
    out_ref[pl.ds(lines, shards, stride=lines + 1), :] = jnp.broadcast_to(kept, (shards, LANES))


def finish_kernel(ids_ref, z_ref, peak_ref, log_ref, part_ref):
    channels, bins = log_ref.shape
    parts = bins // LANES
    own = parts // 2
    step = 2 * parts + 1
    sources = z_ref.shape[0] // step
    lane = lax.broadcasted_iota(jnp.int32, (channels, LANES), 1)
    back = jnp.where(lane == 0, 0, LANES - lane)

    def joined(line, op):
        total = None
        for s in range(0, sources, GROUP):
            term = z_ref[pl.ds(s * step + line, GROUP, stride=step), :]
            total = term if total is None else op(total, term)
        return total

    def in_order(kind, op):
        pieces = []
        for e in range(own):
            pieces.append(joined(kind * parts + e, op))
            mirrored = joined(kind * parts + own + e, op)
            pieces.append(jnp.take_along_axis(mirrored, back, axis=1))
        return jnp.concatenate(pieces, axis=1)

    kept = joined(2 * parts, jnp.add)
    log_mean = in_order(1, jnp.add) / kept[:, :1]
    log_ref[...] = log_mean
    peak_ref[...] = in_order(0, jnp.maximum)
    block = lax.broadcasted_iota(jnp.int32, (BLOCKS, LANES), 0).astype(jnp.float32)
    inside = [block == ids_ref[c : c + 1, :] for c in range(channels)]
    for i in range(parts + 1):
        total = jnp.zeros((BLOCKS, LANES), jnp.float32)
        for c in range(channels):
            term = log_mean[c : c + 1, i * LANES : (i + 1) * LANES] if i < parts else 1.0
            total = total + jnp.where(inside[c], term, 0.0)
        for p in range(part_ref.shape[0]):
            part_ref[p, i * BLOCKS : (i + 1) * BLOCKS, :] = total


def blocks_kernel(parts_ref, out_ref):
    total = parts_ref[0]
    for p in range(1, parts_ref.shape[0]):
        total = total + parts_ref[p]
    counts = total[-BLOCKS:]
    for i in range(out_ref.shape[1] // LANES):
        out_ref[:, i * LANES : (i + 1) * LANES] = total[i * BLOCKS : (i + 1) * BLOCKS] / counts


VMEM = pl.BlockSpec(memory_space=pltpu.VMEM)
SMEM = pl.BlockSpec(memory_space=pltpu.SMEM)
PARAMS = pltpu.CompilerParams(vmem_limit_bytes=48 * 1024 * 1024)


def f32(*shape):
    return jax.ShapeDtypeStruct(shape, jnp.float32)


def on_device(signal, gap_mask, assignment):
    channels, local_time = signal.shape
    shards = lax.axis_size("tm")
    rows = local_time // LANES
    bins = SEG // 2 // shards

    lined = signal.reshape(channels, rows, LANES).transpose(1, 0, 2).reshape(-1, LANES)
    ids, *sent, far, half = pl.pallas_call(
        pack_kernel,
        out_shape=[f32(channels, LANES)]
        + [f32(rows + 8, LANES)] * GROUP
        + [f32(rows // 2 + 8, LANES)],
        in_specs=[SMEM, SMEM, VMEM],
        out_specs=[VMEM] * (GROUP + 2),
        compiler_params=PARAMS,
        name="pack",
    )(gap_mask.T, assignment, lined)

    def moved(x, by):
        return lax.ppermute(x, "tm", [(i, (i + by(i)) % shards) for i in range(shards)])

    far = moved(far, lambda i: REACH if i % 2 else -REACH)
    half = moved(half, lambda i: -REACH if i % 2 else REACH)
    near = [
        x if by == 0 else moved(x, lambda i, by=by: by)
        for by, x in zip(range(1 - REACH, REACH), sent)
    ][::-1]

    lines = 2 * (bins // LANES) + 1
    sums = pl.pallas_call(
        functools.partial(spectra_kernel, shards),
        out_shape=f32(shards * lines, LANES),
        in_specs=[VMEM] * (GROUP + 2),
        out_specs=VMEM,
        scratch_shapes=[
            pltpu.VMEM((2 * ROWS, 3 * LA), jnp.bfloat16),
            pltpu.VMEM((6 * LB, 2 * LB), jnp.bfloat16),
        ],
        compiler_params=PARAMS,
        cost_estimate=pl.CostEstimate(
            flops=4_000_000_000, bytes_accessed=4_000_000, transcendentals=300_000
        ),
        name="spectra",
    )(*near, far, half, tables(shards))
    sums = lax.all_to_all(sums.reshape(shards, 1, -1), "tm", 0, 0, tiled=True)
    peers = lax.axis_size(("chan", "sub"))
    peak_hold, log_mean, part = pl.pallas_call(
        finish_kernel,
        out_shape=[
            f32(channels, bins),
            f32(channels, bins),
            f32(peers, (bins // LANES + 1) * BLOCKS, LANES),
        ],
        in_specs=[VMEM] * 2,
        out_specs=[VMEM] * 3,
        compiler_params=PARAMS,
        name="finish",
    )(ids, sums.reshape(-1, LANES))
    part = lax.all_to_all(part, ("chan", "sub"), 0, 0, tiled=True)
    block_mean = pl.pallas_call(
        blocks_kernel,
        out_shape=f32(BLOCKS, bins),
        in_specs=[VMEM],
        out_specs=VMEM,
        compiler_params=PARAMS,
        name="blocks",
    )(part)
    return peak_hold, log_mean, block_mean


def solution(mesh):
    in_specs = (
        P(("grp", "chan", "sub"), "tm"),
        P(("grp", "chan", "sub"), "tm"),
        P(("grp", "chan", "sub")),
    )
    out_specs = (P(("grp", "chan", "sub"), "tm"), P(("grp", "chan", "sub"), "tm"), P("grp", "tm"))
    return jax.shard_map(
        on_device, mesh=mesh, in_specs=in_specs, out_specs=out_specs, check_vma=False
    )
```

```python
import functools
import math

import jax
import jax.numpy as jnp
import numpy as np
from jax import lax
from jax.experimental import pallas as pl
from jax.experimental.pallas import tpu as pltpu
from jax.sharding import PartitionSpec as P


LA = 256
LB = 128
BLOCKS = 8
SEG = LA * LB
GROUP = 4
ROWS = 144
LANES = 128


def split(x):
    high = x.astype(jnp.bfloat16)
    return high, (x - high.astype(jnp.float32)).astype(jnp.bfloat16)


def owners(shards, role):
    return [
        GROUP * (2 * m + (role + r) % 2) + r
        for m in range(shards // GROUP // 2)
        for r in range(GROUP)
    ]


@functools.lru_cache
def tables(shards):
    k1 = np.arange(ROWS)[:, None]
    angle = 2 * math.pi * ((k1 * np.arange(LA)[None, :]) % LA) / LA
    live = k1 <= LA // 2
    first = np.concatenate([np.cos(angle) * live, -np.sin(angle) * live], axis=0)
    angle = 2 * math.pi * (k1 * np.arange(LB)[None, :]) / SEG
    scale = math.sqrt(1.0 / (0.375 * SEG)) * live
    twiddle = np.cos(angle) * scale, -np.sin(angle) * scale
    own = LB // 2 // shards
    roles = [owners(shards, role) for role in range(2)]
    k2 = [
        k
        for d in map(np.array, roles)
        for k in [own * d + e for e in range(own)] + [LB - 1 - own * d - e for e in range(own)]
    ]
    k2 = np.concatenate(k2)[None, :]
    angle = 2 * math.pi * ((np.arange(LB)[:, None] * k2) % LB) / LB
    c, s = np.cos(angle), -np.sin(angle)
    second = np.concatenate([np.concatenate([c, s], 1), np.concatenate([-s, c], 1)], 0)
    n = np.arange(SEG)
    window = (0.5 - 0.5 * np.cos(2 * math.pi * n / SEG)).reshape(LA, LB)
    halves = [x[:, at : at + LANES] for x in (first, second) for at in (0, LANES)]
    return np.concatenate([*twiddle, window, *halves], axis=0).astype(np.float32)


def pack_kernel(per, mask_ref, assign_ref, x_ref, *refs):
    o_ref, a_ref, b_ref, c_ref, h_ref, ids_ref = refs
    me = lax.axis_index("tm")
    channels = GROUP * per
    rows = x_ref.shape[0] // channels
    half = rows // 2
    even = lax.rem(me, 2) == 0
    for c in range(channels):
        ids_ref[c : c + 1, :] = jnp.full((1, LANES), assign_ref[c].astype(jnp.float32))

    def masks(ref, at, first):
        ref[at : at + 8, :] = jnp.zeros((8, LANES), jnp.float32)
        for c in range(per):
            for s in range(2):
                value = mask_ref[s, first + c].astype(jnp.float32)
                ref[at + 2 * c + s : at + 2 * c + s + 1, :] = jnp.full((1, LANES), value)

    for ref, shift in ((c_ref, 2), (a_ref, 1), (b_ref, GROUP - 1), (o_ref, 0)):
        first = per * lax.rem(me + shift, GROUP)
        for c in range(per):
            ref[c * rows : (c + 1) * rows, :] = x_ref[pl.ds(first + c, rows, stride=channels), :]
        masks(ref, per * rows, first)
    first = per * lax.rem(me + 2, GROUP)
    start = jnp.where(even, half * channels, 0)
    for c in range(per):
        h_ref[c * half : (c + 1) * half, :] = x_ref[
            pl.ds(start + first + c, half, stride=channels), :
        ]
    masks(h_ref, per * half, first)


def powers_of(frames, t_ref, f_ref, w_ref):
    swap = (lax.broadcasted_iota(jnp.int32, (8, LANES), 0) == 0) & (
        lax.rem(lax.broadcasted_iota(jnp.int32, (8, LANES), 1), LB // 2) >= LB // 4
    )
    window = t_ref[2 * ROWS : 2 * ROWS + LA, :]
    framed = []
    for head, tail, live in frames:
        half = head.shape[0]
        tail = tail * window[half:]
        if live is not None:
            tail = tail * live
        framed.append(jnp.concatenate([head * window[:half], tail], axis=0))
    high, low = split(jnp.concatenate(framed, axis=1))
    mid = jnp.dot(
        f_ref[...],
        jnp.concatenate([high, low, high], axis=0),
        preferred_element_type=jnp.float32,
    )
    cosine, sine = t_ref[:ROWS, :], t_ref[ROWS : 2 * ROWS, :]
    turned = []
    for s in range(2):
        re = mid[:ROWS, s * LB : (s + 1) * LB]
        im = mid[ROWS:, s * LB : (s + 1) * LB]
        turned.append(jnp.concatenate([re * cosine - im * sine, re * sine + im * cosine], axis=1))
    high, low = split(jnp.concatenate(turned, axis=0))
    out = jnp.dot(
        jnp.concatenate([high, low, high], axis=1),
        w_ref[...],
        preferred_element_type=jnp.float32,
    )
    powers = out[:, :LB] * out[:, :LB] + out[:, LB:] * out[:, LB:]
    both = []
    for s in range(2):
        mine = powers[s * ROWS : (s + 1) * ROWS]
        first = jnp.where(swap, mine[LA // 2 : LA // 2 + 8], mine[:8])
        both.append(jnp.concatenate([first, mine[8 : LA // 2]], axis=0))
    return both


def live(me, ahead, shards):
    return jnp.where(lax.rem(me + ahead + shards, shards) == 0, 0.0, 1.0)


def spectra_kernel(per, shards, *refs):
    o_ref, a_ref, b_ref, c_ref, t_ref, peak_ref, log_ref, kept_ref, f_ref, w_ref = refs
    at = 2 * ROWS + LA
    side = t_ref[at : at + 2 * ROWS, :], t_ref[at + 2 * ROWS : at + 4 * ROWS, :]
    high, low = split(jnp.concatenate(side, axis=1))
    f_ref[...] = jnp.concatenate([high, high, low], axis=1)
    at += 4 * ROWS
    side = t_ref[at : at + 2 * LB, :], t_ref[at + 2 * LB :, :]
    high, low = split(jnp.concatenate(side, axis=1))
    w_ref[...] = jnp.concatenate([high, high, low], axis=0)
    me = lax.axis_index("tm")
    even = lax.rem(me, 2) == 0
    rows = (o_ref.shape[0] - 8) // per
    half = rows // 2

    def weight(ref, c, s):
        return ref[pl.ds(per * rows + 2 * c + s, 1), :]

    def one_channel(c, carry):
        base = pl.multiple_of(c * rows, rows)

        def halves(ref):
            return ref[pl.ds(base, half), :], ref[pl.ds(base + half, half), :]

        o0, o1 = halves(o_ref)
        a0, a1 = halves(a_ref)
        b0, b1 = halves(b_ref)
        c0, c1 = halves(c_ref)
        pairs = (
            ((c0, c1, None, weight(c_ref, c, 0)), (o0, o1, None, weight(o_ref, c, 0))),
            ((a0, a1, None, weight(a_ref, c, 0)), (a1, o0, live(me, 0, shards), weight(a_ref, c, 1))),
            ((o1, b0, live(me, 1, shards), weight(o_ref, c, 1)), (b0, b1, None, weight(b_ref, c, 0))),
        )
        peak = log_sum = None
        for pair in pairs:
            powers = powers_of([segment[:3] for segment in pair], t_ref, f_ref, w_ref)
            for power, (_, _, _, keep) in zip(powers, pair):
                kept_log = keep * jnp.log(0.25 + power)
                peak = keep * power if peak is None else jnp.maximum(peak, keep * power)
                log_sum = kept_log if log_sum is None else log_sum + kept_log
        at = pl.multiple_of(c * LANES, LANES)
        peak_ref[pl.ds(at, LANES), :] = peak
        log_ref[pl.ds(at, LANES), :] = log_sum
        kept_ref[pl.ds(c, 1), :] = sum(w for pair in pairs for _, _, _, w in pair)
        return carry

    kept_ref[...] = jnp.zeros_like(kept_ref)
    lax.fori_loop(0, per, one_channel, 0)
    crosses = jnp.where(even, live(me, 2, shards), live(me, -1, shards))
    for first in range(0, per, 2):
        frames, keeps = [], []
        for c in range(first, first + 2):
            at = c * rows
            head = jnp.where(even, b_ref[at + half : at + rows, :], c_ref[at + half : at + rows, :])
            tail = jnp.where(even, c_ref[at : at + half, :], a_ref[at : at + half, :])
            frames.append((head, tail, crosses))
            keeps.append(jnp.where(even, weight(b_ref, c, 1), weight(c_ref, c, 1)))
        for i, power in enumerate(powers_of(frames, t_ref, f_ref, w_ref)):
            c, keep = first + i, keeps[i]
            at = slice(c * LANES, (c + 1) * LANES)
            peak_ref[at, :] = jnp.maximum(peak_ref[at, :], keep * power)
            log_ref[at, :] = log_ref[at, :] + keep * jnp.log(0.25 + power)
            kept_ref[c : c + 1, :] = kept_ref[c : c + 1, :] + keep


def chunks_kernel(per, shards, *refs):
    a_ref, b_ref, h_ref, t_ref, peak_ref, log_ref, kept_ref, f_ref, w_ref, keep_ref, send_ref = refs
    me = lax.axis_index("tm")
    even = lax.rem(me, 2) == 0
    role = lax.rem(me // GROUP + lax.rem(me, GROUP), 2)
    rows = (a_ref.shape[0] - 8) // per
    half = rows // 2
    dests = shards // 2
    parts = LB // shards
    lines = 2 * parts * per
    crosses = jnp.where(even, live(me, -1, shards), live(me, 2, shards))
    lane = lax.broadcasted_iota(jnp.int32, (1, LANES), 1)
    kept = jnp.zeros((1, LANES), jnp.float32)
    for first in range(0, per, 2):
        frames, keeps = [], []
        for c in range(first, first + 2):
            at = c * rows
            lent = h_ref[c * half : (c + 1) * half, :]
            head = jnp.where(even, lent, b_ref[at + half : at + rows, :])
            tail = jnp.where(even, a_ref[at : at + half, :], lent)
            frames.append((head, tail, crosses))
            at = per * half + 2 * c + 1
            own = per * rows + 2 * c + 1
            keeps.append(jnp.where(even, h_ref[at : at + 1, :], b_ref[own : own + 1, :]))
        for i, power in enumerate(powers_of(frames, t_ref, f_ref, w_ref)):
            c, keep = first + i, keeps[i]
            at = slice(c * LANES, (c + 1) * LANES)
            peak = jnp.maximum(peak_ref[at, :], keep * power)
            log_sum = log_ref[at, :] + keep * jnp.log(0.25 + power)
            kept = jnp.where(lane == c, kept_ref[c : c + 1, :] + keep, kept)
            for kind, value in enumerate((peak, log_sum)):
                turned = jnp.transpose(value)
                for ref, mine in ((keep_ref, 0), (send_ref, 1)):
                    chosen = jnp.where(role == mine, turned[: LB // 2], turned[LB // 2 :])
                    for part in range(parts):
                        line = (kind * parts + part) * per + c
                        ref[pl.ds(line, dests, stride=lines + 1), :] = chosen[
                            part * dests : (part + 1) * dests
                        ]
    for ref in (keep_ref, send_ref):
        ref[pl.ds(lines, dests, stride=lines + 1), :] = jnp.broadcast_to(kept, (dests, LANES))


def join_kernel(lines, mine_ref, other_ref, out_ref):
    mine, other = mine_ref[...], other_ref[...]
    line = lax.rem(lax.broadcasted_iota(jnp.int32, mine.shape, 0), lines)
    out_ref[...] = jnp.where(line < lines // 2, jnp.maximum(mine, other), mine + other)


def finish_kernel(per, ids_ref, z_ref, peak_ref, log_ref, part_ref):
    channels, bins = log_ref.shape
    parts = bins // LANES
    own = parts // 2
    size = parts * per
    step = 2 * size + 1
    sources = z_ref.shape[0] // step
    lane = lax.broadcasted_iota(jnp.int32, (channels, LANES), 1)
    line = lax.broadcasted_iota(jnp.int32, (channels, LANES), 0)
    back = jnp.where(lane == 0, 0, LANES - lane)

    def joined(r, at, count, op):
        total = None
        for s in range(r, sources, GROUP):
            term = z_ref[s * step + at : s * step + at + count, :]
            total = term if total is None else op(total, term)
        return total

    def in_order(kind, op):
        sets = [joined(r, kind * size, size, op) for r in range(GROUP)]
        pieces = []
        for e in range(own):
            for i, mirrored in ((e, False), (own + e, True)):
                piece = jnp.concatenate([t[i * per : (i + 1) * per] for t in sets], axis=0)
                if mirrored:
                    piece = jnp.take_along_axis(piece, back, axis=1)
                pieces.append(piece)
        return jnp.concatenate(pieces, axis=1)

    kept = jnp.zeros((channels, LANES), jnp.float32)
    for r in range(GROUP):
        row = joined(r, 2 * size, 1, jnp.add)
        kept = jnp.where((line - per * r == lane) & (lane < per), row, kept)
    log_mean = in_order(1, jnp.add) / jnp.sum(kept, axis=1, keepdims=True)
    log_ref[...] = log_mean
    peak_ref[...] = in_order(0, jnp.maximum)
    block = lax.broadcasted_iota(jnp.int32, (BLOCKS, LANES), 0).astype(jnp.float32)
    inside = [block == ids_ref[c : c + 1, :] for c in range(channels)]
    for i in range(parts + 1):
        total = jnp.zeros((BLOCKS, LANES), jnp.float32)
        for c in range(channels):
            term = log_mean[c : c + 1, i * LANES : (i + 1) * LANES] if i < parts else 1.0
            total = total + jnp.where(inside[c], term, 0.0)
        for p in range(part_ref.shape[0]):
            part_ref[p, i * BLOCKS : (i + 1) * BLOCKS, :] = total


def blocks_kernel(parts_ref, out_ref):
    total = parts_ref[0]
    for p in range(1, parts_ref.shape[0]):
        total = total + parts_ref[p]
    counts = total[-BLOCKS:]
    for i in range(out_ref.shape[1] // LANES):
        out_ref[:, i * LANES : (i + 1) * LANES] = total[i * BLOCKS : (i + 1) * BLOCKS] / counts


VMEM = pl.BlockSpec(memory_space=pltpu.VMEM)
SMEM = pl.BlockSpec(memory_space=pltpu.SMEM)
PARAMS = pltpu.CompilerParams(vmem_limit_bytes=48 * 1024 * 1024)


def f32(*shape):
    return jax.ShapeDtypeStruct(shape, jnp.float32)


def on_device(signal, gap_mask, assignment):
    channels, local_time = signal.shape
    shards = lax.axis_size("tm")
    per = channels // GROUP
    rows = local_time // LANES
    bins = SEG // 2 // shards

    lined = signal.reshape(channels, rows, LANES).transpose(1, 0, 2).reshape(-1, LANES)
    whole, small = per * rows + 8, per * rows // 2 + 8
    o, a, b, c, h, ids = pl.pallas_call(
        functools.partial(pack_kernel, per),
        out_shape=[f32(whole, LANES)] * 4 + [f32(small, LANES), f32(channels, LANES)],
        in_specs=[SMEM, SMEM, VMEM],
        out_specs=[VMEM] * 6,
        compiler_params=PARAMS,
        name="pack",
    )(gap_mask.T, assignment, lined)

    def moved(x, by):
        return lax.ppermute(x, "tm", [(i, (i + by(i)) % shards) for i in range(shards)])

    a = moved(a, lambda i: 1)
    b = moved(b, lambda i: -1)
    c = moved(c, lambda i: 2 if i % 2 else -2)
    h = moved(h, lambda i: -2 if i % 2 else 2)

    dests = shards // 2
    lines = 2 * (bins // LANES) * per + 1
    table = tables(shards)
    sums = pl.pallas_call(
        functools.partial(spectra_kernel, per, shards),
        out_shape=[
            f32(per * LANES, LANES),
            f32(per * LANES, LANES),
            f32(8, LANES),
            jax.ShapeDtypeStruct((2 * ROWS, 3 * LA), jnp.bfloat16),
            jax.ShapeDtypeStruct((6 * LB, 2 * LB), jnp.bfloat16),
        ],
        in_specs=[VMEM] * 5,
        out_specs=[VMEM] * 5,
        compiler_params=PARAMS,
        cost_estimate=pl.CostEstimate(
            flops=4_000_000_000, bytes_accessed=4_000_000, transcendentals=300_000
        ),
        name="spectra",
    )(o, a, b, c, table)
    keep, send = pl.pallas_call(
        functools.partial(chunks_kernel, per, shards),
        out_shape=[f32(dests * lines, LANES)] * 2,
        in_specs=[VMEM] * 9,
        out_specs=[VMEM] * 2,
        compiler_params=PARAMS,
        name="chunks",
    )(a, b, h, table, *sums)
    roles = [owners(shards, role) for role in range(2)]
    other = moved(send, lambda i: GROUP if i in roles[0] else -GROUP)
    sums = pl.pallas_call(
        functools.partial(join_kernel, lines),
        out_shape=f32(dests * lines, LANES),
        in_specs=[VMEM] * 2,
        out_specs=VMEM,
        compiler_params=PARAMS,
        name="join",
    )(keep, other)
    sums = lax.all_to_all(
        sums.reshape(dests, 1, -1), "tm", 0, 0, tiled=True, axis_index_groups=roles
    )
    peers = lax.axis_size(("chan", "sub"))
    peak_hold, log_mean, part = pl.pallas_call(
        functools.partial(finish_kernel, per),
        out_shape=[
            f32(channels, bins),
            f32(channels, bins),
            f32(peers, (bins // LANES + 1) * BLOCKS, LANES),
        ],
        in_specs=[VMEM] * 2,
        out_specs=[VMEM] * 3,
        compiler_params=PARAMS,
        name="finish",
    )(ids, sums.reshape(-1, LANES))
    part = lax.all_to_all(part, ("chan", "sub"), 0, 0, tiled=True)
    block_mean = pl.pallas_call(
        blocks_kernel,
        out_shape=f32(BLOCKS, bins),
        in_specs=[VMEM],
        out_specs=VMEM,
        compiler_params=PARAMS,
        name="blocks",
    )(part)
    return peak_hold, log_mean, block_mean


def solution(mesh):
    in_specs = (
        P(("grp", "chan", "sub"), "tm"),
        P(("grp", "chan", "sub"), "tm"),
        P(("grp", "chan", "sub")),
    )
    out_specs = (P(("grp", "chan", "sub"), "tm"), P(("grp", "chan", "sub"), "tm"), P("grp", "tm"))
    return jax.shard_map(
        on_device, mesh=mesh, in_specs=in_specs, out_specs=out_specs, check_vma=False
    )
```

```python
import functools
import math

import jax
import jax.numpy as jnp
import numpy as np
from jax import lax
from jax.experimental import pallas as pl
from jax.experimental.pallas import tpu as pltpu
from jax.sharding import PartitionSpec as P


LA = 256
LB = 128
BLOCKS = 8
SEG = LA * LB
GROUP = 4
ROWS = 144
LANES = 128


def split(x):
    high = x.astype(jnp.bfloat16)
    return high, (x - high.astype(jnp.float32)).astype(jnp.bfloat16)


def owners(shards, role):
    return [
        GROUP * (2 * m + (role + r) % 2) + r
        for m in range(shards // GROUP // 2)
        for r in range(GROUP)
    ]


@functools.lru_cache
def tables(shards):
    k1 = np.arange(ROWS)[:, None]
    angle = 2 * math.pi * ((k1 * np.arange(LA)[None, :]) % LA) / LA
    live = k1 <= LA // 2
    first = np.concatenate([np.cos(angle) * live, -np.sin(angle) * live], axis=0)
    angle = 2 * math.pi * (k1 * np.arange(LB)[None, :]) / SEG
    scale = math.sqrt(1.0 / (0.375 * SEG)) * live
    twiddle = np.cos(angle) * scale, -np.sin(angle) * scale
    own = LB // 2 // shards
    roles = [owners(shards, role) for role in range(2)]
    k2 = [
        k
        for d in map(np.array, roles)
        for k in [own * d + e for e in range(own)] + [LB - 1 - own * d - e for e in range(own)]
    ]
    k2 = np.concatenate(k2)[None, :]
    angle = 2 * math.pi * ((np.arange(LB)[:, None] * k2) % LB) / LB
    c, s = np.cos(angle), -np.sin(angle)
    second = np.concatenate([np.concatenate([c, s], 1), np.concatenate([-s, c], 1)], 0)
    n = np.arange(SEG)
    window = (0.5 - 0.5 * np.cos(2 * math.pi * n / SEG)).reshape(LA, LB)
    halves = [x[:, at : at + LANES] for x in (first, second) for at in (0, LANES)]
    return np.concatenate([*twiddle, window, *halves], axis=0).astype(np.float32)


def pack_kernel(per, mask_ref, assign_ref, x_ref, *refs):
    o_ref, a_ref, b_ref, c_ref, h_ref, ids_ref = refs
    me = lax.axis_index("tm")
    channels = GROUP * per
    rows = x_ref.shape[0] // channels
    half = rows // 2
    even = lax.rem(me, 2) == 0
    for c in range(channels):
        ids_ref[c : c + 1, :] = jnp.full((1, LANES), assign_ref[c].astype(jnp.float32))

    def masks(ref, at, first):
        ref[at : at + 8, :] = jnp.zeros((8, LANES), jnp.float32)
        for c in range(per):
            for s in range(2):
                value = mask_ref[s, first + c].astype(jnp.float32)
                ref[at + 2 * c + s : at + 2 * c + s + 1, :] = jnp.full((1, LANES), value)

    for ref, shift in ((c_ref, 2), (a_ref, 1), (b_ref, GROUP - 1), (o_ref, 0)):
        first = per * lax.rem(me + shift, GROUP)
        for c in range(per):
            ref[c * rows : (c + 1) * rows, :] = x_ref[pl.ds(first + c, rows, stride=channels), :]
        masks(ref, per * rows, first)
    first = per * lax.rem(me + 2, GROUP)
    start = jnp.where(even, half * channels, 0)
    for c in range(per):
        h_ref[c * half : (c + 1) * half, :] = x_ref[
            pl.ds(start + first + c, half, stride=channels), :
        ]
    masks(h_ref, per * half, first)


def powers_of(frames, t_ref, f_ref, w_ref):
    swap = (lax.broadcasted_iota(jnp.int32, (8, LANES), 0) == 0) & (
        lax.rem(lax.broadcasted_iota(jnp.int32, (8, LANES), 1), LB // 2) >= LB // 4
    )
    window = t_ref[2 * ROWS : 2 * ROWS + LA, :]
    framed = []
    for head, tail, live in frames:
        half = head.shape[0]
        tail = tail * window[half:]
        if live is not None:
            tail = tail * live
        framed.append(jnp.concatenate([head * window[:half], tail], axis=0))
    high, low = split(jnp.concatenate(framed, axis=1))
    mid = jnp.dot(
        f_ref[...],
        jnp.concatenate([high, low, high], axis=0),
        preferred_element_type=jnp.float32,
    )
    cosine, sine = t_ref[:ROWS, :], t_ref[ROWS : 2 * ROWS, :]
    turned = []
    for s in range(2):
        re = mid[:ROWS, s * LB : (s + 1) * LB]
        im = mid[ROWS:, s * LB : (s + 1) * LB]
        turned.append(jnp.concatenate([re * cosine - im * sine, re * sine + im * cosine], axis=1))
    high, low = split(jnp.concatenate(turned, axis=0))
    out = jnp.dot(
        jnp.concatenate([high, low, high], axis=1),
        w_ref[...],
        preferred_element_type=jnp.float32,
    )
    powers = out[:, :LB] * out[:, :LB] + out[:, LB:] * out[:, LB:]
    both = []
    for s in range(2):
        mine = powers[s * ROWS : (s + 1) * ROWS]
        first = jnp.where(swap, mine[LA // 2 : LA // 2 + 8], mine[:8])
        both.append(jnp.concatenate([first, mine[8 : LA // 2]], axis=0))
    return both


def live(me, ahead, shards):
    return jnp.where(lax.rem(me + ahead + shards, shards) == 0, 0.0, 1.0)


def add_segments(c, pairs, tabled, sums_refs, fresh=False):
    peak_ref, log_ref, kept_ref = sums_refs
    at = pl.ds(pl.multiple_of(c * LANES, LANES), LANES)
    row = pl.ds(c, 1)
    peak, log_sum, kept = None, None, None
    if not fresh:
        peak, log_sum, kept = peak_ref[at, :], log_ref[at, :], kept_ref[row, :]
    for pair in pairs:
        powers = powers_of([segment[:3] for segment in pair], *tabled)
        for power, (_, _, _, keep) in zip(powers, pair):
            kept_log = keep * jnp.log(0.25 + power)
            peak = keep * power if peak is None else jnp.maximum(peak, keep * power)
            log_sum = kept_log if log_sum is None else log_sum + kept_log
            kept = keep if kept is None else kept + keep
    peak_ref[at, :], log_ref[at, :], kept_ref[row, :] = peak, log_sum, kept


def weight(ref, c, s):
    return ref[pl.ds(ref.shape[0] - 8 + 2 * c + s, 1), :]


def spectra_kernel(per, shards, *refs):
    o_ref, a_ref, c_ref, t_ref, peak_ref, log_ref, kept_ref, f_ref, w_ref = refs
    at = 2 * ROWS + LA
    side = t_ref[at : at + 2 * ROWS, :], t_ref[at + 2 * ROWS : at + 4 * ROWS, :]
    high, low = split(jnp.concatenate(side, axis=1))
    f_ref[...] = jnp.concatenate([high, high, low], axis=1)
    at += 4 * ROWS
    side = t_ref[at : at + 2 * LB, :], t_ref[at + 2 * LB :, :]
    high, low = split(jnp.concatenate(side, axis=1))
    w_ref[...] = jnp.concatenate([high, high, low], axis=0)
    me = lax.axis_index("tm")
    rows = (o_ref.shape[0] - 8) // per
    half = rows // 2

    def one_channel(c, carry):
        base = pl.multiple_of(c * rows, rows)
        (o0, o1), (a0, a1), (c0, c1) = (
            (ref[pl.ds(base, half), :], ref[pl.ds(base + half, half), :])
            for ref in (o_ref, a_ref, c_ref)
        )
        pairs = (
            ((c0, c1, None, weight(c_ref, c, 0)), (o0, o1, None, weight(o_ref, c, 0))),
            (
                (a0, a1, None, weight(a_ref, c, 0)),
                (a1, o0, live(me, 0, shards), weight(a_ref, c, 1)),
            ),
        )
        add_segments(c, pairs, (t_ref, f_ref, w_ref), (peak_ref, log_ref, kept_ref), fresh=True)
        return carry

    kept_ref[...] = jnp.zeros_like(kept_ref)
    lax.fori_loop(0, per, one_channel, 0)


def more_kernel(per, shards, *refs):
    o_ref, a_ref, b_ref, c_ref, t_ref, *old_refs, f_ref, w_ref, peak_ref, log_ref, kept_ref = refs
    sums_refs = peak_ref, log_ref, kept_ref
    for old, new in zip(old_refs, sums_refs):
        new[...] = old[...]
    me = lax.axis_index("tm")
    even = lax.rem(me, 2) == 0
    rows = (o_ref.shape[0] - 8) // per
    half = rows // 2

    def one_channel(c, carry):
        base = pl.multiple_of(c * rows, rows)
        o1 = o_ref[pl.ds(base + half, half), :]
        b0, b1 = b_ref[pl.ds(base, half), :], b_ref[pl.ds(base + half, half), :]
        pairs = (
            (
                (o1, b0, live(me, 1, shards), weight(o_ref, c, 1)),
                (b0, b1, None, weight(b_ref, c, 0)),
            ),
        )
        add_segments(c, pairs, (t_ref, f_ref, w_ref), sums_refs)
        return carry

    lax.fori_loop(0, per, one_channel, 0)
    crosses = jnp.where(even, live(me, 2, shards), live(me, -1, shards))
    for first in range(0, per, 2):
        frames, keeps = [], []
        for c in range(first, first + 2):
            at = c * rows
            head = jnp.where(even, b_ref[at + half : at + rows, :], c_ref[at + half : at + rows, :])
            tail = jnp.where(even, c_ref[at : at + half, :], a_ref[at : at + half, :])
            frames.append((head, tail, crosses))
            keeps.append(jnp.where(even, weight(b_ref, c, 1), weight(c_ref, c, 1)))
        for i, power in enumerate(powers_of(frames, t_ref, f_ref, w_ref)):
            c, keep = first + i, keeps[i]
            at = slice(c * LANES, (c + 1) * LANES)
            peak_ref[at, :] = jnp.maximum(peak_ref[at, :], keep * power)
            log_ref[at, :] = log_ref[at, :] + keep * jnp.log(0.25 + power)
            kept_ref[c : c + 1, :] = kept_ref[c : c + 1, :] + keep


def chunks_kernel(per, shards, *refs):
    a_ref, b_ref, h_ref, t_ref, peak_ref, log_ref, kept_ref, f_ref, w_ref, keep_ref, send_ref = refs
    me = lax.axis_index("tm")
    even = lax.rem(me, 2) == 0
    role = lax.rem(me // GROUP + lax.rem(me, GROUP), 2)
    rows = (a_ref.shape[0] - 8) // per
    half = rows // 2
    dests = shards // 2
    parts = LB // shards
    lines = 2 * parts * per
    crosses = jnp.where(even, live(me, -1, shards), live(me, 2, shards))
    lane = lax.broadcasted_iota(jnp.int32, (1, LANES), 1)
    kept = jnp.zeros((1, LANES), jnp.float32)
    for first in range(0, per, 2):
        frames, keeps = [], []
        for c in range(first, first + 2):
            at = c * rows
            lent = h_ref[c * half : (c + 1) * half, :]
            head = jnp.where(even, lent, b_ref[at + half : at + rows, :])
            tail = jnp.where(even, a_ref[at : at + half, :], lent)
            frames.append((head, tail, crosses))
            at = per * half + 2 * c + 1
            own = per * rows + 2 * c + 1
            keeps.append(jnp.where(even, h_ref[at : at + 1, :], b_ref[own : own + 1, :]))
        for i, power in enumerate(powers_of(frames, t_ref, f_ref, w_ref)):
            c, keep = first + i, keeps[i]
            at = slice(c * LANES, (c + 1) * LANES)
            peak = jnp.maximum(peak_ref[at, :], keep * power)
            log_sum = log_ref[at, :] + keep * jnp.log(0.25 + power)
            kept = jnp.where(lane == c, kept_ref[c : c + 1, :] + keep, kept)
            for kind, value in enumerate((peak, log_sum)):
                turned = jnp.transpose(value)
                for ref, mine in ((keep_ref, 0), (send_ref, 1)):
                    chosen = jnp.where(role == mine, turned[: LB // 2], turned[LB // 2 :])
                    for part in range(parts):
                        line = (kind * parts + part) * per + c
                        ref[pl.ds(line, dests, stride=lines + 1), :] = chosen[
                            part * dests : (part + 1) * dests
                        ]
    for ref in (keep_ref, send_ref):
        ref[pl.ds(lines, dests, stride=lines + 1), :] = jnp.broadcast_to(kept, (dests, LANES))


def join_kernel(lines, mine_ref, other_ref, out_ref):
    mine, other = mine_ref[...], other_ref[...]
    line = lax.rem(lax.broadcasted_iota(jnp.int32, mine.shape, 0), lines)
    out_ref[...] = jnp.where(line < lines // 2, jnp.maximum(mine, other), mine + other)


def finish_kernel(per, ids_ref, z_ref, peak_ref, log_ref, part_ref):
    channels, bins = log_ref.shape
    parts = bins // LANES
    own = parts // 2
    size = parts * per
    step = 2 * size + 1
    sources = z_ref.shape[0] // step
    lane = lax.broadcasted_iota(jnp.int32, (channels, LANES), 1)
    line = lax.broadcasted_iota(jnp.int32, (channels, LANES), 0)
    back = jnp.where(lane == 0, 0, LANES - lane)

    def joined(r, at, count, op):
        total = None
        for s in range(r, sources, GROUP):
            term = z_ref[s * step + at : s * step + at + count, :]
            total = term if total is None else op(total, term)
        return total

    def in_order(kind, op):
        sets = [joined(r, kind * size, size, op) for r in range(GROUP)]
        pieces = []
        for e in range(own):
            for i, mirrored in ((e, False), (own + e, True)):
                piece = jnp.concatenate([t[i * per : (i + 1) * per] for t in sets], axis=0)
                if mirrored:
                    piece = jnp.take_along_axis(piece, back, axis=1)
                pieces.append(piece)
        return jnp.concatenate(pieces, axis=1)

    kept = jnp.zeros((channels, LANES), jnp.float32)
    for r in range(GROUP):
        row = joined(r, 2 * size, 1, jnp.add)
        kept = jnp.where((line - per * r == lane) & (lane < per), row, kept)
    log_mean = in_order(1, jnp.add) / jnp.sum(kept, axis=1, keepdims=True)
    log_ref[...] = log_mean
    peak_ref[...] = in_order(0, jnp.maximum)
    block = lax.broadcasted_iota(jnp.int32, (BLOCKS, LANES), 0).astype(jnp.float32)
    inside = [block == ids_ref[c : c + 1, :] for c in range(channels)]
    for i in range(parts + 1):
        total = jnp.zeros((BLOCKS, LANES), jnp.float32)
        for c in range(channels):
            term = log_mean[c : c + 1, i * LANES : (i + 1) * LANES] if i < parts else 1.0
            total = total + jnp.where(inside[c], term, 0.0)
        for p in range(part_ref.shape[0]):
            part_ref[p, i * BLOCKS : (i + 1) * BLOCKS, :] = total


def blocks_kernel(parts_ref, out_ref):
    total = parts_ref[0]
    for p in range(1, parts_ref.shape[0]):
        total = total + parts_ref[p]
    counts = total[-BLOCKS:]
    for i in range(out_ref.shape[1] // LANES):
        out_ref[:, i * LANES : (i + 1) * LANES] = total[i * BLOCKS : (i + 1) * BLOCKS] / counts


VMEM = pl.BlockSpec(memory_space=pltpu.VMEM)
SMEM = pl.BlockSpec(memory_space=pltpu.SMEM)
PARAMS = pltpu.CompilerParams(vmem_limit_bytes=48 * 1024 * 1024)


def f32(*shape):
    return jax.ShapeDtypeStruct(shape, jnp.float32)


def on_device(signal, gap_mask, assignment):
    channels, local_time = signal.shape
    shards = lax.axis_size("tm")
    per = channels // GROUP
    rows = local_time // LANES
    bins = SEG // 2 // shards

    lined = signal.reshape(channels, rows, LANES).transpose(1, 0, 2).reshape(-1, LANES)
    whole, small = per * rows + 8, per * rows // 2 + 8
    o, a, b, c, h, ids = pl.pallas_call(
        functools.partial(pack_kernel, per),
        out_shape=[f32(whole, LANES)] * 4 + [f32(small, LANES), f32(channels, LANES)],
        in_specs=[SMEM, SMEM, VMEM],
        out_specs=[VMEM] * 6,
        compiler_params=PARAMS,
        name="pack",
    )(gap_mask.T, assignment, lined)

    def moved(x, by):
        return lax.ppermute(x, "tm", [(i, (i + by(i)) % shards) for i in range(shards)])

    a = moved(a, lambda i: 1)
    b = moved(b, lambda i: -1)
    c = moved(c, lambda i: 2 if i % 2 else -2)
    h = moved(h, lambda i: -2 if i % 2 else 2)

    dests = shards // 2
    lines = 2 * (bins // LANES) * per + 1
    table = tables(shards)
    cost = pl.CostEstimate(flops=2_000_000_000, bytes_accessed=2_000_000, transcendentals=150_000)
    sums_shape = [f32(per * LANES, LANES), f32(per * LANES, LANES), f32(8, LANES)]
    *sums, left, right = pl.pallas_call(
        functools.partial(spectra_kernel, per, shards),
        out_shape=[
            *sums_shape,
            jax.ShapeDtypeStruct((2 * ROWS, 3 * LA), jnp.bfloat16),
            jax.ShapeDtypeStruct((6 * LB, 2 * LB), jnp.bfloat16),
        ],
        in_specs=[VMEM] * 4,
        out_specs=[VMEM] * 5,
        compiler_params=PARAMS,
        cost_estimate=cost,
        name="spectra",
    )(o, a, c, table)
    sums = pl.pallas_call(
        functools.partial(more_kernel, per, shards),
        out_shape=sums_shape,
        in_specs=[VMEM] * 10,
        out_specs=[VMEM] * 3,
        compiler_params=PARAMS,
        cost_estimate=cost,
        name="more",
    )(o, a, b, c, table, *sums, left, right)
    keep, send = pl.pallas_call(
        functools.partial(chunks_kernel, per, shards),
        out_shape=[f32(dests * lines, LANES)] * 2,
        in_specs=[VMEM] * 9,
        out_specs=[VMEM] * 2,
        compiler_params=PARAMS,
        name="chunks",
    )(a, b, h, table, *sums, left, right)
    roles = [owners(shards, role) for role in range(2)]
    other = moved(send, lambda i: GROUP if i in roles[0] else -GROUP)
    sums = pl.pallas_call(
        functools.partial(join_kernel, lines),
        out_shape=f32(dests * lines, LANES),
        in_specs=[VMEM] * 2,
        out_specs=VMEM,
        compiler_params=PARAMS,
        name="join",
    )(keep, other)
    sums = lax.all_to_all(
        sums.reshape(dests, 1, -1), "tm", 0, 0, tiled=True, axis_index_groups=roles
    )
    peers = lax.axis_size(("chan", "sub"))
    peak_hold, log_mean, part = pl.pallas_call(
        functools.partial(finish_kernel, per),
        out_shape=[
            f32(channels, bins),
            f32(channels, bins),
            f32(peers, (bins // LANES + 1) * BLOCKS, LANES),
        ],
        in_specs=[VMEM] * 2,
        out_specs=[VMEM] * 3,
        compiler_params=PARAMS,
        name="finish",
    )(ids, sums.reshape(-1, LANES))
    part = lax.all_to_all(part, ("chan", "sub"), 0, 0, tiled=True)
    block_mean = pl.pallas_call(
        blocks_kernel,
        out_shape=f32(BLOCKS, bins),
        in_specs=[VMEM],
        out_specs=VMEM,
        compiler_params=PARAMS,
        name="blocks",
    )(part)
    return peak_hold, log_mean, block_mean


def solution(mesh):
    in_specs = (
        P(("grp", "chan", "sub"), "tm"),
        P(("grp", "chan", "sub"), "tm"),
        P(("grp", "chan", "sub")),
    )
    out_specs = (P(("grp", "chan", "sub"), "tm"), P(("grp", "chan", "sub"), "tm"), P("grp", "tm"))
    return jax.shard_map(
        on_device, mesh=mesh, in_specs=in_specs, out_specs=out_specs, check_vma=False
    )
```

```python
import functools
import math

import jax
import jax.numpy as jnp
import numpy as np
from jax import lax
from jax.experimental import pallas as pl
from jax.experimental.pallas import tpu as pltpu
from jax.sharding import PartitionSpec as P


LA = 256
LB = 128
BLOCKS = 8
SEG = LA * LB
GROUP = 4
ROWS = 144
LANES = 128


def split(x):
    high = x.astype(jnp.bfloat16)
    return high, (x - high.astype(jnp.float32)).astype(jnp.bfloat16)


def owners(shards, role):
    return [
        GROUP * (2 * m + (role + r) % 2) + r
        for m in range(shards // GROUP // 2)
        for r in range(GROUP)
    ]


@functools.lru_cache
def tables(shards):
    k1 = np.arange(ROWS)[:, None]
    angle = 2 * math.pi * ((k1 * np.arange(LA)[None, :]) % LA) / LA
    live = k1 <= LA // 2
    first = np.concatenate([np.cos(angle) * live, -np.sin(angle) * live], axis=0)
    angle = 2 * math.pi * (k1 * np.arange(LB)[None, :]) / SEG
    scale = math.sqrt(1.0 / (0.375 * SEG)) * live
    twiddle = np.cos(angle) * scale, -np.sin(angle) * scale
    own = LB // 2 // shards
    roles = [owners(shards, role) for role in range(2)]
    k2 = [
        k
        for d in map(np.array, roles)
        for k in [own * d + e for e in range(own)] + [LB - 1 - own * d - e for e in range(own)]
    ]
    k2 = np.concatenate(k2)[None, :]
    angle = 2 * math.pi * ((np.arange(LB)[:, None] * k2) % LB) / LB
    c, s = np.cos(angle), -np.sin(angle)
    second = np.concatenate([np.concatenate([c, s], 1), np.concatenate([-s, c], 1)], 0)
    n = np.arange(SEG)
    window = (0.5 - 0.5 * np.cos(2 * math.pi * n / SEG)).reshape(LA, LB)
    halves = [x[:, at : at + LANES] for x in (first, second) for at in (0, LANES)]
    return np.concatenate([*twiddle, window, *halves], axis=0).astype(np.float32)


def pack_kernel(per, mask_ref, assign_ref, x_ref, *refs):
    o_ref, a_ref, b_ref, c_ref, h_ref, ids_ref = refs
    me = lax.axis_index("tm")
    channels = GROUP * per
    rows = x_ref.shape[0] // channels
    half = rows // 2
    even = lax.rem(me, 2) == 0
    for c in range(channels):
        ids_ref[c : c + 1, :] = jnp.full((1, LANES), assign_ref[c].astype(jnp.float32))

    def masks(ref, at, first):
        ref[at : at + 8, :] = jnp.zeros((8, LANES), jnp.float32)
        for c in range(per):
            for s in range(2):
                value = mask_ref[s, first + c].astype(jnp.float32)
                ref[at + 2 * c + s : at + 2 * c + s + 1, :] = jnp.full((1, LANES), value)

    for ref, shift in ((c_ref, 2), (a_ref, 1), (b_ref, GROUP - 1), (o_ref, 0)):
        first = per * lax.rem(me + shift, GROUP)
        for c in range(per):
            ref[c * rows : (c + 1) * rows, :] = x_ref[pl.ds(first + c, rows, stride=channels), :]
        masks(ref, per * rows, first)
    first = per * lax.rem(me + 2, GROUP)
    start = jnp.where(even, half * channels, 0)
    for c in range(per):
        h_ref[c * half : (c + 1) * half, :] = x_ref[
            pl.ds(start + first + c, half, stride=channels), :
        ]
    masks(h_ref, per * half, first)


def powers_of(frames, t_ref, f_ref, w_ref):
    swap = (lax.broadcasted_iota(jnp.int32, (8, LANES), 0) == 0) & (
        lax.rem(lax.broadcasted_iota(jnp.int32, (8, LANES), 1), LB // 2) >= LB // 4
    )
    window = t_ref[2 * ROWS : 2 * ROWS + LA, :]
    framed = []
    for head, tail, live in frames:
        half = head.shape[0]
        tail = tail * window[half:]
        if live is not None:
            tail = tail * live
        framed.append(jnp.concatenate([head * window[:half], tail], axis=0))
    high, low = split(jnp.concatenate(framed, axis=1))
    mid = jnp.dot(
        f_ref[...],
        jnp.concatenate([high, low, high], axis=0),
        preferred_element_type=jnp.float32,
    )
    cosine, sine = t_ref[:ROWS, :], t_ref[ROWS : 2 * ROWS, :]
    turned = []
    for s in range(2):
        re = mid[:ROWS, s * LB : (s + 1) * LB]
        im = mid[ROWS:, s * LB : (s + 1) * LB]
        turned.append(jnp.concatenate([re * cosine - im * sine, re * sine + im * cosine], axis=1))
    high, low = split(jnp.concatenate(turned, axis=0))
    out = jnp.dot(
        jnp.concatenate([high, low, high], axis=1),
        w_ref[...],
        preferred_element_type=jnp.float32,
    )
    powers = out[:, :LB] * out[:, :LB] + out[:, LB:] * out[:, LB:]
    both = []
    for s in range(2):
        mine = powers[s * ROWS : (s + 1) * ROWS]
        first = jnp.where(swap, mine[LA // 2 : LA // 2 + 8], mine[:8])
        both.append(jnp.concatenate([first, mine[8 : LA // 2]], axis=0))
    return both


def live(me, ahead, shards):
    return jnp.where(lax.rem(me + ahead + shards, shards) == 0, 0.0, 1.0)


def spectra_kernel(per, shards, *refs):
    o_ref, a_ref, b_ref, c_ref, t_ref, peak_ref, log_ref, kept_ref, f_ref, w_ref = refs
    at = 2 * ROWS + LA
    side = t_ref[at : at + 2 * ROWS, :], t_ref[at + 2 * ROWS : at + 4 * ROWS, :]
    high, low = split(jnp.concatenate(side, axis=1))
    f_ref[...] = jnp.concatenate([high, high, low], axis=1)
    at += 4 * ROWS
    side = t_ref[at : at + 2 * LB, :], t_ref[at + 2 * LB :, :]
    high, low = split(jnp.concatenate(side, axis=1))
    w_ref[...] = jnp.concatenate([high, high, low], axis=0)
    me = lax.axis_index("tm")
    even = lax.rem(me, 2) == 0
    rows = (o_ref.shape[0] - 8) // per
    half = rows // 2

    def weight(ref, c, s):
        return ref[pl.ds(per * rows + 2 * c + s, 1), :]

    def one_channel(c, carry):
        base = pl.multiple_of(c * rows, rows)

        def halves(ref):
            return ref[pl.ds(base, half), :], ref[pl.ds(base + half, half), :]

        o0, o1 = halves(o_ref)
        a0, a1 = halves(a_ref)
        b0, b1 = halves(b_ref)
        c0, c1 = halves(c_ref)
        pairs = (
            ((c0, c1, None, weight(c_ref, c, 0)), (o0, o1, None, weight(o_ref, c, 0))),
            ((a0, a1, None, weight(a_ref, c, 0)), (a1, o0, live(me, 0, shards), weight(a_ref, c, 1))),
            ((o1, b0, live(me, 1, shards), weight(o_ref, c, 1)), (b0, b1, None, weight(b_ref, c, 0))),
        )
        peak = log_sum = None
        for pair in pairs:
            powers = powers_of([segment[:3] for segment in pair], t_ref, f_ref, w_ref)
            for power, (_, _, _, keep) in zip(powers, pair):
                kept_log = keep * jnp.log(0.25 + power)
                peak = keep * power if peak is None else jnp.maximum(peak, keep * power)
                log_sum = kept_log if log_sum is None else log_sum + kept_log
        at = pl.multiple_of(c * LANES, LANES)
        peak_ref[pl.ds(at, LANES), :] = peak
        log_ref[pl.ds(at, LANES), :] = log_sum
        kept_ref[pl.ds(c, 1), :] = sum(w for pair in pairs for _, _, _, w in pair)
        return carry

    kept_ref[...] = jnp.zeros_like(kept_ref)
    lax.fori_loop(0, per, one_channel, 0)
    crosses = jnp.where(even, live(me, 2, shards), live(me, -1, shards))
    for first in range(0, per, 2):
        frames, keeps = [], []
        for c in range(first, first + 2):
            at = c * rows
            head = jnp.where(even, b_ref[at + half : at + rows, :], c_ref[at + half : at + rows, :])
            tail = jnp.where(even, c_ref[at : at + half, :], a_ref[at : at + half, :])
            frames.append((head, tail, crosses))
            keeps.append(jnp.where(even, weight(b_ref, c, 1), weight(c_ref, c, 1)))
        for i, power in enumerate(powers_of(frames, t_ref, f_ref, w_ref)):
            c, keep = first + i, keeps[i]
            at = slice(c * LANES, (c + 1) * LANES)
            peak_ref[at, :] = jnp.maximum(peak_ref[at, :], keep * power)
            log_ref[at, :] = log_ref[at, :] + keep * jnp.log(0.25 + power)
            kept_ref[c : c + 1, :] = kept_ref[c : c + 1, :] + keep


def chunks_kernel(per, shards, *refs):
    a_ref, b_ref, h_ref, t_ref, peak_ref, log_ref, kept_ref, f_ref, w_ref, keep_ref, send_ref = refs
    me = lax.axis_index("tm")
    even = lax.rem(me, 2) == 0
    role = lax.rem(me // GROUP + lax.rem(me, GROUP), 2)
    rows = (a_ref.shape[0] - 8) // per
    half = rows // 2
    dests = shards // 2
    parts = LB // shards
    lines = 2 * parts * per
    crosses = jnp.where(even, live(me, -1, shards), live(me, 2, shards))
    lane = lax.broadcasted_iota(jnp.int32, (1, LANES), 1)
    kept = jnp.zeros((1, LANES), jnp.float32)
    for first in range(0, per, 2):
        frames, keeps = [], []
        for c in range(first, first + 2):
            at = c * rows
            lent = h_ref[c * half : (c + 1) * half, :]
            head = jnp.where(even, lent, b_ref[at + half : at + rows, :])
            tail = jnp.where(even, a_ref[at : at + half, :], lent)
            frames.append((head, tail, crosses))
            at = per * half + 2 * c + 1
            own = per * rows + 2 * c + 1
            keeps.append(jnp.where(even, h_ref[at : at + 1, :], b_ref[own : own + 1, :]))
        for i, power in enumerate(powers_of(frames, t_ref, f_ref, w_ref)):
            c, keep = first + i, keeps[i]
            at = slice(c * LANES, (c + 1) * LANES)
            peak = jnp.maximum(peak_ref[at, :], keep * power)
            log_sum = log_ref[at, :] + keep * jnp.log(0.25 + power)
            kept = jnp.where(lane == c, kept_ref[c : c + 1, :] + keep, kept)
            for kind, value in enumerate((peak, log_sum)):
                turned = jnp.transpose(value)
                for ref, mine in ((keep_ref, 0), (send_ref, 1)):
                    chosen = jnp.where(role == mine, turned[: LB // 2], turned[LB // 2 :])
                    for part in range(parts):
                        line = (kind * parts + part) * per + c
                        ref[pl.ds(line, dests, stride=lines + 1), :] = chosen[
                            part * dests : (part + 1) * dests
                        ]
    for ref in (keep_ref, send_ref):
        ref[pl.ds(lines, dests, stride=lines + 1), :] = jnp.broadcast_to(kept, (dests, LANES))


def join_kernel(lines, mine_ref, other_ref, out_ref):
    mine, other = mine_ref[...], other_ref[...]
    line = lax.rem(lax.broadcasted_iota(jnp.int32, mine.shape, 0), lines)
    out_ref[...] = jnp.where(line < lines // 2, jnp.maximum(mine, other), mine + other)


def finish_kernel(per, ids_ref, z_ref, peak_ref, log_ref, part_ref):
    channels, bins = log_ref.shape
    parts = bins // LANES
    own = parts // 2
    size = parts * per
    step = 2 * size + 1
    sources = z_ref.shape[0] // step
    lane = lax.broadcasted_iota(jnp.int32, (channels, LANES), 1)
    line = lax.broadcasted_iota(jnp.int32, (channels, LANES), 0)
    back = jnp.where(lane == 0, 0, LANES - lane)

    def joined(r, at, count, op):
        total = None
        for s in range(r, sources, GROUP):
            term = z_ref[s * step + at : s * step + at + count, :]
            total = term if total is None else op(total, term)
        return total

    def in_order(kind, op):
        sets = [joined(r, kind * size, size, op) for r in range(GROUP)]
        pieces = []
        for e in range(own):
            for i, mirrored in ((e, False), (own + e, True)):
                piece = jnp.concatenate([t[i * per : (i + 1) * per] for t in sets], axis=0)
                if mirrored:
                    piece = jnp.take_along_axis(piece, back, axis=1)
                pieces.append(piece)
        return jnp.concatenate(pieces, axis=1)

    kept = jnp.zeros((channels, LANES), jnp.float32)
    for r in range(GROUP):
        row = joined(r, 2 * size, 1, jnp.add)
        kept = jnp.where((line - per * r == lane) & (lane < per), row, kept)
    log_mean = in_order(1, jnp.add) / jnp.sum(kept, axis=1, keepdims=True)
    log_ref[...] = log_mean
    peak_ref[...] = in_order(0, jnp.maximum)
    block = lax.broadcasted_iota(jnp.int32, (BLOCKS, LANES), 0).astype(jnp.float32)
    inside = [block == ids_ref[c : c + 1, :] for c in range(channels)]
    step = parts * BLOCKS + 1
    peers = part_ref.shape[0] // step
    for i in range(parts):
        total = jnp.zeros((BLOCKS, LANES), jnp.float32)
        for c in range(channels):
            term = log_mean[c : c + 1, i * LANES : (i + 1) * LANES]
            total = total + jnp.where(inside[c], term, 0.0)
        for p in range(peers):
            at = p * step + i * BLOCKS
            part_ref[at : at + BLOCKS, :] = total
    matches = jnp.where(ids_ref[...] == lane.astype(jnp.float32), 1.0, 0.0)
    counts = jnp.sum(matches, axis=0, keepdims=True)
    for p in range(peers):
        at = p * step + parts * BLOCKS
        part_ref[at : at + 1, :] = counts


def blocks_kernel(parts_ref, out_ref):
    parts = out_ref.shape[1] // LANES
    step = parts * BLOCKS + 1
    peers = parts_ref.shape[0] // step

    def total(at, count):
        value = parts_ref[at : at + count, :]
        for p in range(1, peers):
            value = value + parts_ref[p * step + at : p * step + at + count, :]
        return value

    lane = lax.broadcasted_iota(jnp.int32, (BLOCKS, LANES), 1)
    block = lax.broadcasted_iota(jnp.int32, (BLOCKS, LANES), 0)
    row = total(parts * BLOCKS, 1)
    counts = jnp.sum(jnp.where(lane == block, row, 0.0), axis=1, keepdims=True)
    for i in range(parts):
        out_ref[:, i * LANES : (i + 1) * LANES] = total(i * BLOCKS, BLOCKS) / counts


VMEM = pl.BlockSpec(memory_space=pltpu.VMEM)
SMEM = pl.BlockSpec(memory_space=pltpu.SMEM)
PARAMS = pltpu.CompilerParams(vmem_limit_bytes=48 * 1024 * 1024)


def f32(*shape):
    return jax.ShapeDtypeStruct(shape, jnp.float32)


def on_device(signal, gap_mask, assignment):
    channels, local_time = signal.shape
    shards = lax.axis_size("tm")
    per = channels // GROUP
    rows = local_time // LANES
    bins = SEG // 2 // shards

    lined = signal.reshape(channels, rows, LANES).transpose(1, 0, 2).reshape(-1, LANES)
    whole, small = per * rows + 8, per * rows // 2 + 8
    o, a, b, c, h, ids = pl.pallas_call(
        functools.partial(pack_kernel, per),
        out_shape=[f32(whole, LANES)] * 4 + [f32(small, LANES), f32(channels, LANES)],
        in_specs=[SMEM, SMEM, VMEM],
        out_specs=[VMEM] * 6,
        compiler_params=PARAMS,
        name="pack",
    )(gap_mask.T, assignment, lined)

    def moved(x, by):
        return lax.ppermute(x, "tm", [(i, (i + by(i)) % shards) for i in range(shards)])

    a = moved(a, lambda i: 1)
    b = moved(b, lambda i: -1)
    c = moved(c, lambda i: 2 if i % 2 else -2)
    h = moved(h, lambda i: -2 if i % 2 else 2)

    dests = shards // 2
    lines = 2 * (bins // LANES) * per + 1
    table = tables(shards)
    sums = pl.pallas_call(
        functools.partial(spectra_kernel, per, shards),
        out_shape=[
            f32(per * LANES, LANES),
            f32(per * LANES, LANES),
            f32(8, LANES),
            jax.ShapeDtypeStruct((2 * ROWS, 3 * LA), jnp.bfloat16),
            jax.ShapeDtypeStruct((6 * LB, 2 * LB), jnp.bfloat16),
        ],
        in_specs=[VMEM] * 5,
        out_specs=[VMEM] * 5,
        compiler_params=PARAMS,
        cost_estimate=pl.CostEstimate(
            flops=4_000_000_000, bytes_accessed=4_000_000, transcendentals=300_000
        ),
        name="spectra",
    )(o, a, b, c, table)
    keep, send = pl.pallas_call(
        functools.partial(chunks_kernel, per, shards),
        out_shape=[f32(dests * lines, LANES)] * 2,
        in_specs=[VMEM] * 9,
        out_specs=[VMEM] * 2,
        compiler_params=PARAMS,
        name="chunks",
    )(a, b, h, table, *sums)
    roles = [owners(shards, role) for role in range(2)]
    other = moved(send, lambda i: GROUP if i in roles[0] else -GROUP)
    sums = pl.pallas_call(
        functools.partial(join_kernel, lines),
        out_shape=f32(dests * lines, LANES),
        in_specs=[VMEM] * 2,
        out_specs=VMEM,
        compiler_params=PARAMS,
        name="join",
    )(keep, other)
    sums = lax.all_to_all(
        sums.reshape(dests, 1, -1), "tm", 0, 0, tiled=True, axis_index_groups=roles
    )
    peers = lax.axis_size(("chan", "sub"))
    peak_hold, log_mean, part = pl.pallas_call(
        functools.partial(finish_kernel, per),
        out_shape=[
            f32(channels, bins),
            f32(channels, bins),
            f32(peers * (bins // LANES * BLOCKS + 1), LANES),
        ],
        in_specs=[VMEM] * 2,
        out_specs=[VMEM] * 3,
        compiler_params=PARAMS,
        name="finish",
    )(ids, sums.reshape(-1, LANES))
    part = lax.all_to_all(part.reshape(peers, 1, -1), ("chan", "sub"), 0, 0, tiled=True)
    block_mean = pl.pallas_call(
        blocks_kernel,
        out_shape=f32(BLOCKS, bins),
        in_specs=[VMEM],
        out_specs=VMEM,
        compiler_params=PARAMS,
        name="blocks",
    )(part.reshape(-1, LANES))
    return peak_hold, log_mean, block_mean


def solution(mesh):
    in_specs = (
        P(("grp", "chan", "sub"), "tm"),
        P(("grp", "chan", "sub"), "tm"),
        P(("grp", "chan", "sub")),
    )
    out_specs = (P(("grp", "chan", "sub"), "tm"), P(("grp", "chan", "sub"), "tm"), P("grp", "tm"))
    return jax.shard_map(
        on_device, mesh=mesh, in_specs=in_specs, out_specs=out_specs, check_vma=False
    )
```

```python
import functools
import math

import jax
import jax.numpy as jnp
import numpy as np
from jax import lax
from jax.experimental import pallas as pl
from jax.experimental.pallas import tpu as pltpu
from jax.sharding import PartitionSpec as P


LA = 256
LB = 128
BLOCKS = 8
SEG = LA * LB
GROUP = 4
ROWS = 144
LANES = 128


def split(x):
    high = x.astype(jnp.bfloat16)
    return high, (x - high.astype(jnp.float32)).astype(jnp.bfloat16)


def owners(shards, role):
    return [
        GROUP * (2 * m + (role + r) % 2) + r
        for m in range(shards // GROUP // 2)
        for r in range(GROUP)
    ]


@functools.lru_cache
def tables(shards):
    k1 = np.arange(ROWS)[:, None]
    angle = 2 * math.pi * ((k1 * np.arange(LA)[None, :]) % LA) / LA
    live = k1 <= LA // 2
    first = np.concatenate([np.cos(angle) * live, -np.sin(angle) * live], axis=0)
    angle = 2 * math.pi * (k1 * np.arange(LB)[None, :]) / SEG
    scale = math.sqrt(1.0 / (0.375 * SEG)) * live
    twiddle = np.cos(angle) * scale, -np.sin(angle) * scale
    own = LB // 2 // shards
    roles = [owners(shards, role) for role in range(2)]
    k2 = [
        k
        for d in map(np.array, roles)
        for k in [own * d + e for e in range(own)] + [LB - 1 - own * d - e for e in range(own)]
    ]
    k2 = np.concatenate(k2)[None, :]
    angle = 2 * math.pi * ((np.arange(LB)[:, None] * k2) % LB) / LB
    c, s = np.cos(angle), -np.sin(angle)
    second = np.concatenate([np.concatenate([c, s], 1), np.concatenate([-s, c], 1)], 0)
    n = np.arange(SEG)
    window = (0.5 - 0.5 * np.cos(2 * math.pi * n / SEG)).reshape(LA, LB)
    halves = [x[:, at : at + LANES] for x in (first, second) for at in (0, LANES)]
    return np.concatenate([*twiddle, window, *halves], axis=0).astype(np.float32)


def pack_kernel(per, mask_ref, assign_ref, x_ref, *refs):
    o_ref, a_ref, b_ref, c_ref, h_ref, ids_ref = refs
    me = lax.axis_index("tm")
    channels = GROUP * per
    rows = x_ref.shape[0] // channels
    half = rows // 2
    even = lax.rem(me, 2) == 0
    for c in range(channels):
        ids_ref[c : c + 1, :] = jnp.full((1, LANES), assign_ref[c].astype(jnp.float32))

    def masks(ref, at, first):
        ref[at : at + 8, :] = jnp.zeros((8, LANES), jnp.float32)
        for c in range(per):
            for s in range(2):
                value = mask_ref[s, first + c].astype(jnp.float32)
                ref[at + 2 * c + s : at + 2 * c + s + 1, :] = jnp.full((1, LANES), value)

    for ref, shift in ((c_ref, 2), (a_ref, 1), (b_ref, GROUP - 1), (o_ref, 0)):
        first = per * lax.rem(me + shift, GROUP)
        for c in range(per):
            ref[c * rows : (c + 1) * rows, :] = x_ref[pl.ds(first + c, rows, stride=channels), :]
        masks(ref, per * rows, first)
    first = per * lax.rem(me + 2, GROUP)
    start = jnp.where(even, half * channels, 0)
    for c in range(per):
        h_ref[c * half : (c + 1) * half, :] = x_ref[
            pl.ds(start + first + c, half, stride=channels), :
        ]
    masks(h_ref, per * half, first)


def powers_of(frames, t_ref, f_ref, w_ref):
    swap = (lax.broadcasted_iota(jnp.int32, (8, LANES), 0) == 0) & (
        lax.rem(lax.broadcasted_iota(jnp.int32, (8, LANES), 1), LB // 2) >= LB // 4
    )
    window = t_ref[2 * ROWS : 2 * ROWS + LA, :]
    framed = []
    for head, tail, live in frames:
        half = head.shape[0]
        tail = tail * window[half:]
        if live is not None:
            tail = tail * live
        framed.append(jnp.concatenate([head * window[:half], tail], axis=0))
    high, low = split(jnp.concatenate(framed, axis=1))
    mid = jnp.dot(
        f_ref[...],
        jnp.concatenate([high, low, high], axis=0),
        preferred_element_type=jnp.float32,
    )
    cosine, sine = t_ref[:ROWS, :], t_ref[ROWS : 2 * ROWS, :]
    turned = []
    for s in range(2):
        re = mid[:ROWS, s * LB : (s + 1) * LB]
        im = mid[ROWS:, s * LB : (s + 1) * LB]
        turned.append(jnp.concatenate([re * cosine - im * sine, re * sine + im * cosine], axis=1))
    high, low = split(jnp.concatenate(turned, axis=0))
    out = jnp.dot(
        jnp.concatenate([high, low, high], axis=1),
        w_ref[...],
        preferred_element_type=jnp.float32,
    )
    powers = out[:, :LB] * out[:, :LB] + out[:, LB:] * out[:, LB:]
    both = []
    for s in range(2):
        mine = powers[s * ROWS : (s + 1) * ROWS]
        first = jnp.where(swap, mine[LA // 2 : LA // 2 + 8], mine[:8])
        both.append(jnp.concatenate([first, mine[8 : LA // 2]], axis=0))
    return both


def live(me, ahead, shards):
    return jnp.where(lax.rem(me + ahead + shards, shards) == 0, 0.0, 1.0)


def spectra_kernel(per, shards, *refs):
    o_ref, a_ref, b_ref, c_ref, t_ref, peak_ref, log_ref, kept_ref, f_ref, w_ref = refs
    at = 2 * ROWS + LA
    side = t_ref[at : at + 2 * ROWS, :], t_ref[at + 2 * ROWS : at + 4 * ROWS, :]
    high, low = split(jnp.concatenate(side, axis=1))
    f_ref[...] = jnp.concatenate([high, high, low], axis=1)
    at += 4 * ROWS
    side = t_ref[at : at + 2 * LB, :], t_ref[at + 2 * LB :, :]
    high, low = split(jnp.concatenate(side, axis=1))
    w_ref[...] = jnp.concatenate([high, high, low], axis=0)
    me = lax.axis_index("tm")
    even = lax.rem(me, 2) == 0
    rows = (o_ref.shape[0] - 8) // per
    half = rows // 2

    def weight(ref, c, s):
        return ref[pl.ds(per * rows + 2 * c + s, 1), :]

    def one_channel(c, carry):
        base = pl.multiple_of(c * rows, rows)

        def halves(ref):
            return ref[pl.ds(base, half), :], ref[pl.ds(base + half, half), :]

        o0, o1 = halves(o_ref)
        a0, a1 = halves(a_ref)
        b0, b1 = halves(b_ref)
        c0, c1 = halves(c_ref)
        pairs = (
            ((c0, c1, None, weight(c_ref, c, 0)), (o0, o1, None, weight(o_ref, c, 0))),
            ((a0, a1, None, weight(a_ref, c, 0)), (a1, o0, live(me, 0, shards), weight(a_ref, c, 1))),
            ((o1, b0, live(me, 1, shards), weight(o_ref, c, 1)), (b0, b1, None, weight(b_ref, c, 0))),
        )
        peak = log_sum = None
        for pair in pairs:
            powers = powers_of([segment[:3] for segment in pair], t_ref, f_ref, w_ref)
            for power, (_, _, _, keep) in zip(powers, pair):
                kept_log = keep * jnp.log(0.25 + power)
                peak = keep * power if peak is None else jnp.maximum(peak, keep * power)
                log_sum = kept_log if log_sum is None else log_sum + kept_log
        at = pl.multiple_of(c * LANES, LANES)
        peak_ref[pl.ds(at, LANES), :] = peak
        log_ref[pl.ds(at, LANES), :] = log_sum
        kept_ref[pl.ds(c, 1), :] = sum(w for pair in pairs for _, _, _, w in pair)
        return carry

    kept_ref[...] = jnp.zeros_like(kept_ref)
    lax.fori_loop(0, per, one_channel, 0)
    crosses = jnp.where(even, live(me, 2, shards), live(me, -1, shards))
    for first in range(0, per, 2):
        frames, keeps = [], []
        for c in range(first, first + 2):
            at = c * rows
            head = jnp.where(even, b_ref[at + half : at + rows, :], c_ref[at + half : at + rows, :])
            tail = jnp.where(even, c_ref[at : at + half, :], a_ref[at : at + half, :])
            frames.append((head, tail, crosses))
            keeps.append(jnp.where(even, weight(b_ref, c, 1), weight(c_ref, c, 1)))
        for i, power in enumerate(powers_of(frames, t_ref, f_ref, w_ref)):
            c, keep = first + i, keeps[i]
            at = slice(c * LANES, (c + 1) * LANES)
            peak_ref[at, :] = jnp.maximum(peak_ref[at, :], keep * power)
            log_ref[at, :] = log_ref[at, :] + keep * jnp.log(0.25 + power)
            kept_ref[c : c + 1, :] = kept_ref[c : c + 1, :] + keep


def chunks_kernel(per, shards, *refs):
    a_ref, b_ref, h_ref, t_ref, peak_ref, log_ref, kept_ref, f_ref, w_ref, keep_ref, send_ref = refs
    me = lax.axis_index("tm")
    even = lax.rem(me, 2) == 0
    role = lax.rem(me // GROUP + lax.rem(me, GROUP), 2)
    rows = (a_ref.shape[0] - 8) // per
    half = rows // 2
    dests = shards // 2
    parts = LB // shards
    lines = 2 * parts * per
    crosses = jnp.where(even, live(me, -1, shards), live(me, 2, shards))
    lane = lax.broadcasted_iota(jnp.int32, (1, LANES), 1)
    kept = jnp.zeros((1, LANES), jnp.float32)
    for first in range(0, per, 2):
        frames, keeps = [], []
        for c in range(first, first + 2):
            at = c * rows
            lent = h_ref[c * half : (c + 1) * half, :]
            head = jnp.where(even, lent, b_ref[at + half : at + rows, :])
            tail = jnp.where(even, a_ref[at : at + half, :], lent)
            frames.append((head, tail, crosses))
            at = per * half + 2 * c + 1
            own = per * rows + 2 * c + 1
            keeps.append(jnp.where(even, h_ref[at : at + 1, :], b_ref[own : own + 1, :]))
        for i, power in enumerate(powers_of(frames, t_ref, f_ref, w_ref)):
            c, keep = first + i, keeps[i]
            at = slice(c * LANES, (c + 1) * LANES)
            peak = jnp.maximum(peak_ref[at, :], keep * power)
            log_sum = log_ref[at, :] + keep * jnp.log(0.25 + power)
            kept = jnp.where(lane == c, kept_ref[c : c + 1, :] + keep, kept)
            for kind, value in enumerate((peak, log_sum)):
                turned = jnp.transpose(value)
                for ref, mine in ((keep_ref, 0), (send_ref, 1)):
                    chosen = jnp.where(role == mine, turned[: LB // 2], turned[LB // 2 :])
                    for part in range(parts):
                        line = (kind * parts + part) * per + c
                        ref[pl.ds(line, dests, stride=lines + 1), :] = chosen[
                            part * dests : (part + 1) * dests
                        ]
    for ref in (keep_ref, send_ref):
        ref[pl.ds(lines, dests, stride=lines + 1), :] = jnp.broadcast_to(kept, (dests, LANES))


def join_kernel(lines, mine_ref, other_ref, out_ref):
    mine, other = mine_ref[...], other_ref[...]
    line = lax.rem(lax.broadcasted_iota(jnp.int32, mine.shape, 0), lines)
    out_ref[...] = jnp.where(line < lines // 2, jnp.maximum(mine, other), mine + other)


def joined(z_ref, step, r, at, count, op):
    total = None
    for s in range(r, z_ref.shape[0] // step, GROUP):
        term = z_ref[s * step + at : s * step + at + count, :]
        total = term if total is None else op(total, term)
    return total


def in_order(per, parts, z_ref, kind, op):
    own = parts // 2
    size = parts * per
    lane = lax.broadcasted_iota(jnp.int32, (GROUP * per, LANES), 1)
    back = jnp.where(lane == 0, 0, LANES - lane)
    sets = [joined(z_ref, 2 * size + 1, r, kind * size, size, op) for r in range(GROUP)]
    pieces = []
    for e in range(own):
        for i, mirrored in ((e, False), (own + e, True)):
            piece = jnp.concatenate([t[i * per : (i + 1) * per] for t in sets], axis=0)
            if mirrored:
                piece = jnp.take_along_axis(piece, back, axis=1)
            pieces.append(piece)
    return jnp.concatenate(pieces, axis=1)


def peaks_kernel(per, z_ref, peak_ref):
    peak_ref[...] = in_order(per, peak_ref.shape[1] // LANES, z_ref, 0, jnp.maximum)


def finish_kernel(per, ids_ref, z_ref, log_ref, part_ref):
    channels, bins = log_ref.shape
    parts = bins // LANES
    size = parts * per
    lane = lax.broadcasted_iota(jnp.int32, (channels, LANES), 1)
    line = lax.broadcasted_iota(jnp.int32, (channels, LANES), 0)
    kept = jnp.zeros((channels, LANES), jnp.float32)
    for r in range(GROUP):
        row = joined(z_ref, 2 * size + 1, r, 2 * size, 1, jnp.add)
        kept = jnp.where((line - per * r == lane) & (lane < per), row, kept)
    log_mean = in_order(per, parts, z_ref, 1, jnp.add) / jnp.sum(kept, axis=1, keepdims=True)
    log_ref[...] = log_mean
    block = lax.broadcasted_iota(jnp.int32, (BLOCKS, LANES), 0).astype(jnp.float32)
    inside = [block == ids_ref[c : c + 1, :] for c in range(channels)]
    step = parts * BLOCKS + 1
    peers = part_ref.shape[0] // step
    for i in range(parts):
        total = jnp.zeros((BLOCKS, LANES), jnp.float32)
        for c in range(channels):
            term = log_mean[c : c + 1, i * LANES : (i + 1) * LANES]
            total = total + jnp.where(inside[c], term, 0.0)
        for p in range(peers):
            at = p * step + i * BLOCKS
            part_ref[at : at + BLOCKS, :] = total
    matches = jnp.where(ids_ref[...] == lane.astype(jnp.float32), 1.0, 0.0)
    counts = jnp.sum(matches, axis=0, keepdims=True)
    for p in range(peers):
        at = p * step + parts * BLOCKS
        part_ref[at : at + 1, :] = counts


def blocks_kernel(parts_ref, out_ref):
    parts = out_ref.shape[1] // LANES
    step = parts * BLOCKS + 1
    peers = parts_ref.shape[0] // step

    def total(at, count):
        value = parts_ref[at : at + count, :]
        for p in range(1, peers):
            value = value + parts_ref[p * step + at : p * step + at + count, :]
        return value

    lane = lax.broadcasted_iota(jnp.int32, (BLOCKS, LANES), 1)
    block = lax.broadcasted_iota(jnp.int32, (BLOCKS, LANES), 0)
    row = total(parts * BLOCKS, 1)
    counts = jnp.sum(jnp.where(lane == block, row, 0.0), axis=1, keepdims=True)
    for i in range(parts):
        out_ref[:, i * LANES : (i + 1) * LANES] = total(i * BLOCKS, BLOCKS) / counts


VMEM = pl.BlockSpec(memory_space=pltpu.VMEM)
SMEM = pl.BlockSpec(memory_space=pltpu.SMEM)
PARAMS = pltpu.CompilerParams(vmem_limit_bytes=48 * 1024 * 1024)


def f32(*shape):
    return jax.ShapeDtypeStruct(shape, jnp.float32)


def on_device(signal, gap_mask, assignment):
    channels, local_time = signal.shape
    shards = lax.axis_size("tm")
    per = channels // GROUP
    rows = local_time // LANES
    bins = SEG // 2 // shards

    lined = signal.reshape(channels, rows, LANES).transpose(1, 0, 2).reshape(-1, LANES)
    whole, small = per * rows + 8, per * rows // 2 + 8
    o, a, b, c, h, ids = pl.pallas_call(
        functools.partial(pack_kernel, per),
        out_shape=[f32(whole, LANES)] * 4 + [f32(small, LANES), f32(channels, LANES)],
        in_specs=[SMEM, SMEM, VMEM],
        out_specs=[VMEM] * 6,
        compiler_params=PARAMS,
        name="pack",
    )(gap_mask.T, assignment, lined)

    def moved(x, by):
        return lax.ppermute(x, "tm", [(i, (i + by(i)) % shards) for i in range(shards)])

    a = moved(a, lambda i: 1)
    b = moved(b, lambda i: -1)
    c = moved(c, lambda i: 2 if i % 2 else -2)
    h = moved(h, lambda i: -2 if i % 2 else 2)

    dests = shards // 2
    lines = 2 * (bins // LANES) * per + 1
    table = tables(shards)
    sums = pl.pallas_call(
        functools.partial(spectra_kernel, per, shards),
        out_shape=[
            f32(per * LANES, LANES),
            f32(per * LANES, LANES),
            f32(8, LANES),
            jax.ShapeDtypeStruct((2 * ROWS, 3 * LA), jnp.bfloat16),
            jax.ShapeDtypeStruct((6 * LB, 2 * LB), jnp.bfloat16),
        ],
        in_specs=[VMEM] * 5,
        out_specs=[VMEM] * 5,
        compiler_params=PARAMS,
        cost_estimate=pl.CostEstimate(
            flops=4_000_000_000, bytes_accessed=4_000_000, transcendentals=300_000
        ),
        name="spectra",
    )(o, a, b, c, table)
    keep, send = pl.pallas_call(
        functools.partial(chunks_kernel, per, shards),
        out_shape=[f32(dests * lines, LANES)] * 2,
        in_specs=[VMEM] * 9,
        out_specs=[VMEM] * 2,
        compiler_params=PARAMS,
        name="chunks",
    )(a, b, h, table, *sums)
    roles = [owners(shards, role) for role in range(2)]
    other = moved(send, lambda i: GROUP if i in roles[0] else -GROUP)
    sums = pl.pallas_call(
        functools.partial(join_kernel, lines),
        out_shape=f32(dests * lines, LANES),
        in_specs=[VMEM] * 2,
        out_specs=VMEM,
        compiler_params=PARAMS,
        name="join",
    )(keep, other)
    sums = lax.all_to_all(
        sums.reshape(dests, 1, -1), "tm", 0, 0, tiled=True, axis_index_groups=roles
    )
    peers = lax.axis_size(("chan", "sub"))
    sums = sums.reshape(-1, LANES)
    log_mean, part = pl.pallas_call(
        functools.partial(finish_kernel, per),
        out_shape=[
            f32(channels, bins),
            f32(peers * (bins // LANES * BLOCKS + 1), LANES),
        ],
        in_specs=[VMEM] * 2,
        out_specs=[VMEM] * 2,
        compiler_params=PARAMS,
        name="finish",
    )(ids, sums)
    part = lax.all_to_all(part.reshape(peers, 1, -1), ("chan", "sub"), 0, 0, tiled=True)
    peak_hold = pl.pallas_call(
        functools.partial(peaks_kernel, per),
        out_shape=f32(channels, bins),
        in_specs=[VMEM],
        out_specs=VMEM,
        compiler_params=PARAMS,
        cost_estimate=pl.CostEstimate(flops=20_000_000, bytes_accessed=200_000, transcendentals=0),
        name="peaks",
    )(sums)
    block_mean = pl.pallas_call(
        blocks_kernel,
        out_shape=f32(BLOCKS, bins),
        in_specs=[VMEM],
        out_specs=VMEM,
        compiler_params=PARAMS,
        name="blocks",
    )(part.reshape(-1, LANES))
    return peak_hold, log_mean, block_mean


def solution(mesh):
    in_specs = (
        P(("grp", "chan", "sub"), "tm"),
        P(("grp", "chan", "sub"), "tm"),
        P(("grp", "chan", "sub")),
    )
    out_specs = (P(("grp", "chan", "sub"), "tm"), P(("grp", "chan", "sub"), "tm"), P("grp", "tm"))
    return jax.shard_map(
        on_device, mesh=mesh, in_specs=in_specs, out_specs=out_specs, check_vma=False
    )
```

```python
import functools
import math

import jax
import jax.numpy as jnp
import numpy as np
from jax import lax
from jax.experimental import pallas as pl
from jax.experimental.pallas import tpu as pltpu
from jax.sharding import PartitionSpec as P


LA = 256
LB = 128
BLOCKS = 8
SEG = LA * LB
GROUP = 4
ROWS = 144
LANES = 128


def split(x):
    high = x.astype(jnp.bfloat16)
    return high, (x - high.astype(jnp.float32)).astype(jnp.bfloat16)


def owners(shards, role):
    return [
        GROUP * (2 * m + (role + r) % 2) + r
        for m in range(shards // GROUP // 2)
        for r in range(GROUP)
    ]


@functools.lru_cache
def tables(shards):
    k1 = np.arange(ROWS)[:, None]
    angle = 2 * math.pi * ((k1 * np.arange(LA)[None, :]) % LA) / LA
    live = k1 <= LA // 2
    first = np.concatenate([np.cos(angle) * live, -np.sin(angle) * live], axis=0)
    angle = 2 * math.pi * (k1 * np.arange(LB)[None, :]) / SEG
    scale = math.sqrt(1.0 / (0.375 * SEG)) * live
    twiddle = np.cos(angle) * scale, -np.sin(angle) * scale
    own = LB // 2 // shards
    roles = [owners(shards, role) for role in range(2)]
    k2 = [
        k
        for d in map(np.array, roles)
        for k in [own * d + e for e in range(own)] + [LB - 1 - own * d - e for e in range(own)]
    ]
    k2 = np.concatenate(k2)[None, :]
    angle = 2 * math.pi * ((np.arange(LB)[:, None] * k2) % LB) / LB
    c, s = np.cos(angle), -np.sin(angle)
    second = np.concatenate([np.concatenate([c, s], 1), np.concatenate([-s, c], 1)], 0)
    n = np.arange(SEG)
    window = (0.5 - 0.5 * np.cos(2 * math.pi * n / SEG)).reshape(LA, LB)
    halves = [x[:, at : at + LANES] for x in (first, second) for at in (0, LANES)]
    return np.concatenate([*twiddle, window, *halves], axis=0).astype(np.float32)


def pack_kernel(per, far, mask_ref, assign_ref, x_ref, *refs):
    c_ref = refs[0] if far else None
    o_ref, a_ref, b_ref, h_ref, ids_ref = (None,) * 5 if far else refs
    me = lax.axis_index("tm")
    channels = GROUP * per
    rows = x_ref.shape[0] // channels
    half = rows // 2
    even = lax.rem(me, 2) == 0
    for c in range(0 if far else channels):
        ids_ref[c : c + 1, :] = jnp.full((1, LANES), assign_ref[c].astype(jnp.float32))

    def masks(ref, at, first):
        ref[at : at + 8, :] = jnp.zeros((8, LANES), jnp.float32)
        for c in range(per):
            for s in range(2):
                value = mask_ref[s, first + c].astype(jnp.float32)
                ref[at + 2 * c + s : at + 2 * c + s + 1, :] = jnp.full((1, LANES), value)

    for ref, shift in ((c_ref, 2), (a_ref, 1), (b_ref, GROUP - 1), (o_ref, 0)):
        if (ref is c_ref) != far:
            continue
        first = per * lax.rem(me + shift, GROUP)
        for c in range(per):
            ref[c * rows : (c + 1) * rows, :] = x_ref[pl.ds(first + c, rows, stride=channels), :]
        masks(ref, per * rows, first)
    if far:
        return
    first = per * lax.rem(me + 2, GROUP)
    start = jnp.where(even, half * channels, 0)
    for c in range(per):
        h_ref[c * half : (c + 1) * half, :] = x_ref[
            pl.ds(start + first + c, half, stride=channels), :
        ]
    masks(h_ref, per * half, first)


def powers_of(frames, t_ref, f_ref, w_ref):
    swap = (lax.broadcasted_iota(jnp.int32, (8, LANES), 0) == 0) & (
        lax.rem(lax.broadcasted_iota(jnp.int32, (8, LANES), 1), LB // 2) >= LB // 4
    )
    window = t_ref[2 * ROWS : 2 * ROWS + LA, :]
    framed = []
    for head, tail, live in frames:
        half = head.shape[0]
        tail = tail * window[half:]
        if live is not None:
            tail = tail * live
        framed.append(jnp.concatenate([head * window[:half], tail], axis=0))
    high, low = split(jnp.concatenate(framed, axis=1))
    mid = jnp.dot(
        f_ref[...],
        jnp.concatenate([high, low, high], axis=0),
        preferred_element_type=jnp.float32,
    )
    cosine, sine = t_ref[:ROWS, :], t_ref[ROWS : 2 * ROWS, :]
    turned = []
    for s in range(2):
        re = mid[:ROWS, s * LB : (s + 1) * LB]
        im = mid[ROWS:, s * LB : (s + 1) * LB]
        turned.append(jnp.concatenate([re * cosine - im * sine, re * sine + im * cosine], axis=1))
    high, low = split(jnp.concatenate(turned, axis=0))
    out = jnp.dot(
        jnp.concatenate([high, low, high], axis=1),
        w_ref[...],
        preferred_element_type=jnp.float32,
    )
    powers = out[:, :LB] * out[:, :LB] + out[:, LB:] * out[:, LB:]
    both = []
    for s in range(2):
        mine = powers[s * ROWS : (s + 1) * ROWS]
        first = jnp.where(swap, mine[LA // 2 : LA // 2 + 8], mine[:8])
        both.append(jnp.concatenate([first, mine[8 : LA // 2]], axis=0))
    return both


def live(me, ahead, shards):
    return jnp.where(lax.rem(me + ahead + shards, shards) == 0, 0.0, 1.0)


def spectra_kernel(per, shards, *refs):
    o_ref, a_ref, b_ref, c_ref, t_ref, peak_ref, log_ref, kept_ref, f_ref, w_ref = refs
    at = 2 * ROWS + LA
    side = t_ref[at : at + 2 * ROWS, :], t_ref[at + 2 * ROWS : at + 4 * ROWS, :]
    high, low = split(jnp.concatenate(side, axis=1))
    f_ref[...] = jnp.concatenate([high, high, low], axis=1)
    at += 4 * ROWS
    side = t_ref[at : at + 2 * LB, :], t_ref[at + 2 * LB :, :]
    high, low = split(jnp.concatenate(side, axis=1))
    w_ref[...] = jnp.concatenate([high, high, low], axis=0)
    me = lax.axis_index("tm")
    even = lax.rem(me, 2) == 0
    rows = (o_ref.shape[0] - 8) // per
    half = rows // 2

    def weight(ref, c, s):
        return ref[pl.ds(per * rows + 2 * c + s, 1), :]

    def one_channel(c, carry):
        base = pl.multiple_of(c * rows, rows)

        def halves(ref):
            return ref[pl.ds(base, half), :], ref[pl.ds(base + half, half), :]

        o0, o1 = halves(o_ref)
        a0, a1 = halves(a_ref)
        b0, b1 = halves(b_ref)
        c0, c1 = halves(c_ref)
        pairs = (
            ((c0, c1, None, weight(c_ref, c, 0)), (o0, o1, None, weight(o_ref, c, 0))),
            ((a0, a1, None, weight(a_ref, c, 0)), (a1, o0, live(me, 0, shards), weight(a_ref, c, 1))),
            ((o1, b0, live(me, 1, shards), weight(o_ref, c, 1)), (b0, b1, None, weight(b_ref, c, 0))),
        )
        peak = log_sum = None
        for pair in pairs:
            powers = powers_of([segment[:3] for segment in pair], t_ref, f_ref, w_ref)
            for power, (_, _, _, keep) in zip(powers, pair):
                kept_log = keep * jnp.log(0.25 + power)
                peak = keep * power if peak is None else jnp.maximum(peak, keep * power)
                log_sum = kept_log if log_sum is None else log_sum + kept_log
        at = pl.multiple_of(c * LANES, LANES)
        peak_ref[pl.ds(at, LANES), :] = peak
        log_ref[pl.ds(at, LANES), :] = log_sum
        kept_ref[pl.ds(c, 1), :] = sum(w for pair in pairs for _, _, _, w in pair)
        return carry

    kept_ref[...] = jnp.zeros_like(kept_ref)
    lax.fori_loop(0, per, one_channel, 0)
    crosses = jnp.where(even, live(me, 2, shards), live(me, -1, shards))
    for first in range(0, per, 2):
        frames, keeps = [], []
        for c in range(first, first + 2):
            at = c * rows
            head = jnp.where(even, b_ref[at + half : at + rows, :], c_ref[at + half : at + rows, :])
            tail = jnp.where(even, c_ref[at : at + half, :], a_ref[at : at + half, :])
            frames.append((head, tail, crosses))
            keeps.append(jnp.where(even, weight(b_ref, c, 1), weight(c_ref, c, 1)))
        for i, power in enumerate(powers_of(frames, t_ref, f_ref, w_ref)):
            c, keep = first + i, keeps[i]
            at = slice(c * LANES, (c + 1) * LANES)
            peak_ref[at, :] = jnp.maximum(peak_ref[at, :], keep * power)
            log_ref[at, :] = log_ref[at, :] + keep * jnp.log(0.25 + power)
            kept_ref[c : c + 1, :] = kept_ref[c : c + 1, :] + keep


def chunks_kernel(per, shards, *refs):
    a_ref, b_ref, h_ref, t_ref, peak_ref, log_ref, kept_ref, f_ref, w_ref, keep_ref, send_ref = refs
    me = lax.axis_index("tm")
    even = lax.rem(me, 2) == 0
    role = lax.rem(me // GROUP + lax.rem(me, GROUP), 2)
    rows = (a_ref.shape[0] - 8) // per
    half = rows // 2
    dests = shards // 2
    parts = LB // shards
    lines = 2 * parts * per
    crosses = jnp.where(even, live(me, -1, shards), live(me, 2, shards))
    lane = lax.broadcasted_iota(jnp.int32, (1, LANES), 1)
    kept = jnp.zeros((1, LANES), jnp.float32)
    for first in range(0, per, 2):
        frames, keeps = [], []
        for c in range(first, first + 2):
            at = c * rows
            lent = h_ref[c * half : (c + 1) * half, :]
            head = jnp.where(even, lent, b_ref[at + half : at + rows, :])
            tail = jnp.where(even, a_ref[at : at + half, :], lent)
            frames.append((head, tail, crosses))
            at = per * half + 2 * c + 1
            own = per * rows + 2 * c + 1
            keeps.append(jnp.where(even, h_ref[at : at + 1, :], b_ref[own : own + 1, :]))
        for i, power in enumerate(powers_of(frames, t_ref, f_ref, w_ref)):
            c, keep = first + i, keeps[i]
            at = slice(c * LANES, (c + 1) * LANES)
            peak = jnp.maximum(peak_ref[at, :], keep * power)
            log_sum = log_ref[at, :] + keep * jnp.log(0.25 + power)
            kept = jnp.where(lane == c, kept_ref[c : c + 1, :] + keep, kept)
            for kind, value in enumerate((peak, log_sum)):
                turned = jnp.transpose(value)
                for ref, mine in ((keep_ref, 0), (send_ref, 1)):
                    chosen = jnp.where(role == mine, turned[: LB // 2], turned[LB // 2 :])
                    for part in range(parts):
                        line = (kind * parts + part) * per + c
                        ref[pl.ds(line, dests, stride=lines + 1), :] = chosen[
                            part * dests : (part + 1) * dests
                        ]
    for ref in (keep_ref, send_ref):
        ref[pl.ds(lines, dests, stride=lines + 1), :] = jnp.broadcast_to(kept, (dests, LANES))


def join_kernel(lines, mine_ref, other_ref, out_ref):
    mine, other = mine_ref[...], other_ref[...]
    line = lax.rem(lax.broadcasted_iota(jnp.int32, mine.shape, 0), lines)
    out_ref[...] = jnp.where(line < lines // 2, jnp.maximum(mine, other), mine + other)


def finish_kernel(per, ids_ref, z_ref, peak_ref, log_ref, part_ref):
    channels, bins = log_ref.shape
    parts = bins // LANES
    own = parts // 2
    size = parts * per
    step = 2 * size + 1
    sources = z_ref.shape[0] // step
    lane = lax.broadcasted_iota(jnp.int32, (channels, LANES), 1)
    line = lax.broadcasted_iota(jnp.int32, (channels, LANES), 0)
    back = jnp.where(lane == 0, 0, LANES - lane)

    def joined(r, at, count, op):
        total = None
        for s in range(r, sources, GROUP):
            term = z_ref[s * step + at : s * step + at + count, :]
            total = term if total is None else op(total, term)
        return total

    def in_order(kind, op):
        sets = [joined(r, kind * size, size, op) for r in range(GROUP)]
        pieces = []
        for e in range(own):
            for i, mirrored in ((e, False), (own + e, True)):
                piece = jnp.concatenate([t[i * per : (i + 1) * per] for t in sets], axis=0)
                if mirrored:
                    piece = jnp.take_along_axis(piece, back, axis=1)
                pieces.append(piece)
        return jnp.concatenate(pieces, axis=1)

    kept = jnp.zeros((channels, LANES), jnp.float32)
    for r in range(GROUP):
        row = joined(r, 2 * size, 1, jnp.add)
        kept = jnp.where((line - per * r == lane) & (lane < per), row, kept)
    log_mean = in_order(1, jnp.add) / jnp.sum(kept, axis=1, keepdims=True)
    log_ref[...] = log_mean
    peak_ref[...] = in_order(0, jnp.maximum)
    block = lax.broadcasted_iota(jnp.int32, (BLOCKS, LANES), 0).astype(jnp.float32)
    inside = [block == ids_ref[c : c + 1, :] for c in range(channels)]
    step = parts * BLOCKS + 1
    peers = part_ref.shape[0] // step
    for i in range(parts):
        total = jnp.zeros((BLOCKS, LANES), jnp.float32)
        for c in range(channels):
            term = log_mean[c : c + 1, i * LANES : (i + 1) * LANES]
            total = total + jnp.where(inside[c], term, 0.0)
        for p in range(peers):
            at = p * step + i * BLOCKS
            part_ref[at : at + BLOCKS, :] = total
    matches = jnp.where(ids_ref[...] == lane.astype(jnp.float32), 1.0, 0.0)
    counts = jnp.sum(matches, axis=0, keepdims=True)
    for p in range(peers):
        at = p * step + parts * BLOCKS
        part_ref[at : at + 1, :] = counts


def blocks_kernel(parts_ref, out_ref):
    parts = out_ref.shape[1] // LANES
    step = parts * BLOCKS + 1
    peers = parts_ref.shape[0] // step

    def total(at, count):
        value = parts_ref[at : at + count, :]
        for p in range(1, peers):
            value = value + parts_ref[p * step + at : p * step + at + count, :]
        return value

    lane = lax.broadcasted_iota(jnp.int32, (BLOCKS, LANES), 1)
    block = lax.broadcasted_iota(jnp.int32, (BLOCKS, LANES), 0)
    row = total(parts * BLOCKS, 1)
    counts = jnp.sum(jnp.where(lane == block, row, 0.0), axis=1, keepdims=True)
    for i in range(parts):
        out_ref[:, i * LANES : (i + 1) * LANES] = total(i * BLOCKS, BLOCKS) / counts


VMEM = pl.BlockSpec(memory_space=pltpu.VMEM)
SMEM = pl.BlockSpec(memory_space=pltpu.SMEM)
PARAMS = pltpu.CompilerParams(vmem_limit_bytes=48 * 1024 * 1024)


def f32(*shape):
    return jax.ShapeDtypeStruct(shape, jnp.float32)


def on_device(signal, gap_mask, assignment):
    channels, local_time = signal.shape
    shards = lax.axis_size("tm")
    per = channels // GROUP
    rows = local_time // LANES
    bins = SEG // 2 // shards

    lined = signal.reshape(channels, rows, LANES).transpose(1, 0, 2).reshape(-1, LANES)
    whole, small = per * rows + 8, per * rows // 2 + 8

    def packed(far, shapes):
        return pl.pallas_call(
            functools.partial(pack_kernel, per, far),
            out_shape=shapes,
            in_specs=[SMEM, SMEM, VMEM],
            out_specs=[VMEM] * len(shapes),
            compiler_params=PARAMS,
            name="pack",
        )(gap_mask.T, assignment, lined)

    def moved(x, by):
        return lax.ppermute(x, "tm", [(i, (i + by(i)) % shards) for i in range(shards)])

    (c,) = packed(True, [f32(whole, LANES)])
    o, a, b, h, ids = packed(
        False, [f32(whole, LANES)] * 3 + [f32(small, LANES), f32(channels, LANES)]
    )
    a = moved(a, lambda i: 1)
    b = moved(b, lambda i: -1)
    c = moved(c, lambda i: 2 if i % 2 else -2)
    h = moved(h, lambda i: -2 if i % 2 else 2)

    dests = shards // 2
    lines = 2 * (bins // LANES) * per + 1
    table = tables(shards)
    sums = pl.pallas_call(
        functools.partial(spectra_kernel, per, shards),
        out_shape=[
            f32(per * LANES, LANES),
            f32(per * LANES, LANES),
            f32(8, LANES),
            jax.ShapeDtypeStruct((2 * ROWS, 3 * LA), jnp.bfloat16),
            jax.ShapeDtypeStruct((6 * LB, 2 * LB), jnp.bfloat16),
        ],
        in_specs=[VMEM] * 5,
        out_specs=[VMEM] * 5,
        compiler_params=PARAMS,
        cost_estimate=pl.CostEstimate(
            flops=4_000_000_000, bytes_accessed=4_000_000, transcendentals=300_000
        ),
        name="spectra",
    )(o, a, b, c, table)
    keep, send = pl.pallas_call(
        functools.partial(chunks_kernel, per, shards),
        out_shape=[f32(dests * lines, LANES)] * 2,
        in_specs=[VMEM] * 9,
        out_specs=[VMEM] * 2,
        compiler_params=PARAMS,
        name="chunks",
    )(a, b, h, table, *sums)
    roles = [owners(shards, role) for role in range(2)]
    other = moved(send, lambda i: GROUP if i in roles[0] else -GROUP)
    sums = pl.pallas_call(
        functools.partial(join_kernel, lines),
        out_shape=f32(dests * lines, LANES),
        in_specs=[VMEM] * 2,
        out_specs=VMEM,
        compiler_params=PARAMS,
        name="join",
    )(keep, other)
    sums = lax.all_to_all(
        sums.reshape(dests, 1, -1), "tm", 0, 0, tiled=True, axis_index_groups=roles
    )
    peers = lax.axis_size(("chan", "sub"))
    peak_hold, log_mean, part = pl.pallas_call(
        functools.partial(finish_kernel, per),
        out_shape=[
            f32(channels, bins),
            f32(channels, bins),
            f32(peers * (bins // LANES * BLOCKS + 1), LANES),
        ],
        in_specs=[VMEM] * 2,
        out_specs=[VMEM] * 3,
        compiler_params=PARAMS,
        name="finish",
    )(ids, sums.reshape(-1, LANES))
    part = lax.all_to_all(part.reshape(peers, 1, -1), ("chan", "sub"), 0, 0, tiled=True)
    block_mean = pl.pallas_call(
        blocks_kernel,
        out_shape=f32(BLOCKS, bins),
        in_specs=[VMEM],
        out_specs=VMEM,
        compiler_params=PARAMS,
        name="blocks",
    )(part.reshape(-1, LANES))
    return peak_hold, log_mean, block_mean


def solution(mesh):
    in_specs = (
        P(("grp", "chan", "sub"), "tm"),
        P(("grp", "chan", "sub"), "tm"),
        P(("grp", "chan", "sub")),
    )
    out_specs = (P(("grp", "chan", "sub"), "tm"), P(("grp", "chan", "sub"), "tm"), P("grp", "tm"))
    return jax.shard_map(
        on_device, mesh=mesh, in_specs=in_specs, out_specs=out_specs, check_vma=False
    )
```
